256 devices in a mesh: down: 32 (over y, z_lo, core), cross: 8 (over x, z_hi).
Axes of the slice: x: 4, y: 4, z: 8 (z_hi: 2, z_lo: 4; z = z_hi * 4 + z_lo), core: 2. Of those that a mesh axis runs over, the one named last changes fastest.
Arguments:
- position: float32 [3, 16384, 128], P(None, ('down', 'cross')), may hold values from 0.5 to 4.5, as said below
- velocity: float32 [3, 16384, 128], P(None, ('down', 'cross')), may hold values from -6 to 6
- affine: float32 [9, 16384, 128], P(None, ('down', 'cross')), may hold values from -3 to 3
- deform: float32 [9, 16384, 128], P(None, ('down', 'cross')), may hold values from -0.1 to 1.2, as said below
- particle_mass: float32 [16384, 128], P(('down', 'cross')), may hold values from 0.5 to 2
- block_count: int32 [16384], P(('down', 'cross')), may hold values from 0 to 128, as said below
- block_brick: int32 [16384], P(('down', 'cross')), may hold values from 0 to 2047
- boundary_mask: int32 [512, 128, 128], P('down', 'cross'), may hold values 0 or 1
- leaving_block: int32 [16384], P(('down', 'cross')), may hold values from 0 to 63, as said below
- leaving_dest: int32 [16384], P(('down', 'cross')), may hold values from 0 to 8, as said below
Outputs:
- new_state: float32 [24, 16384, 128], P(None, ('down', 'cross'))
- arrivals: float32 [25, 16384, 128], P(None, ('down', 'cross'))
The draws below stay inside these ranges and needn't reach their ends.
Inputs may be any that keep to these rules, and one draw needn't show every extreme that they name: `position`: component 0 lies in 0.5 to 2 + 0.5, component 1 in 0.5 to 2 + 0.5, component 2 in 0.5 to 4 + 0.5. `deform`: rows 0, 4 and 8 (the diagonal) lie in 0.8 to 1.2, the other rows in -0.1 to 0.1. `block_count`: the first block of every device holds 128 live particles. `leaving_block`: the entries of one device name distinct blocks. `leaving_dest`: id 4 marks an unused entry; no device names one id more than 8 times; every device names id 7 exactly 8 times; in every draw each neighbour of some device names the id that points to that device 8 times.
All inputs are finite; a program needn't handle non-finite values. No bound on the sum of `boundary_mask` on one device may be relied on, other than what follows from the above.
Results may differ from the reference program's by a relative error of at most 0.0003.
Values sent between devices are 32-bit elements; how exact they have to be, the bound alone decides.
A program may use at most 64 MiB of HBM per device.

```python
import math
import jax
import jax.numpy as jnp
from jax import lax

GX = 16
GY = 16
GZ = 128
BLOCKS = 64
SLOTS = 128
BX = 2
BY = 2
BZ = 4
MIG = 8
NBX = 8
NBY = 8
NBRICK = 2048
NX = 512
NY = 128
LIST = 64
ROWS = 16384
N_DOWN = 32
N_CROSS = 8


def draw_position(key, part):
    shape = (ROWS, SLOTS)
    pieces = []
    for component, extent in enumerate((BX, BY, BZ)):
        sample = jax.random.uniform(jax.random.fold_in(key, component), shape, jnp.float32)
        pieces.append(0.5 + extent * 0.999 * sample)
    return jnp.stack(pieces)


def draw_deform(key, part):
    shape = (ROWS, SLOTS)
    pieces = []
    for component in range(9):
        subkey = jax.random.fold_in(key, 40 + component)
        if component % 4 == 0:
            drawn_values = jax.random.uniform(subkey, shape, jnp.float32, 0.85, 1.15)
        else:
            drawn_values = jax.random.uniform(subkey, shape, jnp.float32, -0.1, 0.1)
        pieces.append(drawn_values)
    return jnp.stack(pieces)


def draw_block_count(key, part):
    row_ids = jnp.arange(ROWS, dtype=jnp.int32)
    down_index = row_ids // BLOCKS // N_CROSS
    lowest = SLOTS // 2 * down_index // max(N_DOWN - 1, 1)
    drawn_values = jax.random.randint(jax.random.fold_in(key, 60), (ROWS,), 0, SLOTS + 1, dtype=jnp.int32)
    counts = jnp.maximum(drawn_values, lowest)
    return jnp.where(row_ids % BLOCKS == 0, SLOTS, counts).astype(jnp.int32)


def crossing_lists(key):
    devices = N_DOWN * N_CROSS
    key_load = jax.random.fold_in(key, 101)
    key_pick = jax.random.fold_in(key, 102)
    key_order = jax.random.fold_in(key, 103)
    key_block = jax.random.fold_in(key, 104)
    steps_down = jnp.array([-1, -1, -1, 0, 0, 1, 1, 1], jnp.int32)
    steps_cross = jnp.array([-1, 0, 1, -1, 1, -1, 0, 1], jnp.int32)
    caps_low = jnp.array([0, 0, 0, 0, 0, MIG // 4, MIG, MIG // 4], jnp.int32)
    caps_high = jnp.array([MIG // 4] * 3 + [MIG // 2] * 2 + [MIG] * 3, jnp.int32) + 1
    load_table = jax.random.randint(key_load, (devices, 8), caps_low, caps_high, dtype=jnp.int32)
    target = jax.random.randint(key_pick, (), 0, devices, dtype=jnp.int32)
    device_ids = jnp.arange(devices, dtype=jnp.int32)
    own_down = device_ids // N_CROSS
    own_cross = device_ids % N_CROSS
    aims_here = (own_down[:, None] + steps_down[None, :] == target // N_CROSS) & (own_cross[:, None] + steps_cross[None, :] == target % N_CROSS)
    load_table = jnp.where(aims_here, MIG, load_table)
    move_ids = jnp.array([0, 1, 2, 3, 5, 6, 7, 8], jnp.int32)
    entry_ids = jnp.arange(LIST, dtype=jnp.int32)
    slot_rank = entry_ids % MIG
    slot_move = entry_ids // MIG
    used_slots = slot_rank[None, :] < load_table[:, slot_move]
    dest_ids = jnp.where(used_slots, move_ids[slot_move][None, :], 4)
    scores = jax.random.randint(key_order, (devices, LIST), 0, 1 << 20, dtype=jnp.int32) * LIST + entry_ids[None, :]
    entry_order = jnp.argsort(scores, axis=1)
    dest_ids = jnp.take_along_axis(dest_ids, entry_order, axis=1)
    block_scores = jax.random.randint(key_block, (devices, BLOCKS), 0, 1 << 20, dtype=jnp.int32) * BLOCKS + jnp.arange(BLOCKS, dtype=jnp.int32)[None, :]
    chosen = jnp.argsort(block_scores, axis=1)[:, :LIST]
    return (chosen.reshape(-1).astype(jnp.int32), dest_ids.reshape(-1).astype(jnp.int32))


def draw_leaving_block(key, part):
    return crossing_lists(jax.random.fold_in(key, 5))[0]


def draw_leaving_dest(key, part):
    return crossing_lists(jax.random.fold_in(key, 5))[1]


def set_ends(entries, own_key, least, top_value):
    longest = entries.shape.index(max(entries.shape))
    spots = []
    for shift in (0, 1):
        where = [jax.random.randint(jax.random.fold_in(own_key, axis), (), 0, length) for axis, length in enumerate(entries.shape)]
        where[longest] = (where[longest] + shift) % entries.shape[longest]
        spots.append(tuple(where))
    return entries.at[spots[0]].set(least).at[spots[1]].set(top_value)


def level_of(own_key, shape, cuts, least, largest):
    def one(dim, blocks):
        draws = jax.random.uniform(jax.random.fold_in(jax.random.fold_in(own_key, 6), dim), (blocks,), jnp.float32, least / len(cuts), largest / len(cuts))
        return jnp.repeat(jnp.exp(draws), shape[dim] // blocks).reshape((-1,) + (1,) * (len(shape) - dim - 1))

    factor_of = one(*cuts[0])
    for cut in cuts[1:]:
        factor_of = factor_of * one(*cut)
    return factor_of


def gaussian(key, dims, width, limit, cuts=(), kind=jnp.bfloat16):
    values = width * jax.random.normal(key, dims, jnp.float32)
    if cuts:
        values = values * level_of(key, dims, cuts, -0.22, 0.18)
    return jnp.clip(values, -limit, limit).astype(kind)


def setup_inputs(seed: int = 0) -> dict:
    arg_keys = jax.random.split(jax.random.key(seed), 11)
    position = draw_position(jax.random.fold_in(arg_keys[10], 71), 0)
    velocity = gaussian(arg_keys[1], (3, ROWS, SLOTS), 1.0, 6.0, ((1, 256),), jnp.float32)
    affine = gaussian(arg_keys[2], (9, ROWS, SLOTS), 0.3, 3.0, ((1, 256),), jnp.float32)
    deform = draw_deform(jax.random.fold_in(arg_keys[10], 71), 0)
    particle_mass = jnp.clip(jnp.exp(math.log(2.0) - 1.3862944 * jax.random.uniform(arg_keys[4], (ROWS, SLOTS), jnp.float32) ** level_of(arg_keys[4], (ROWS, SLOTS), ((0, 256),), -0.2, 0.2)), 0.5, 2.0)
    block_count = draw_block_count(jax.random.fold_in(arg_keys[10], 71), 0)
    block_brick = set_ends(jax.random.randint(arg_keys[6], (ROWS,), 0, NBRICK), jax.random.fold_in(arg_keys[6], 1), 0, NBRICK - 1).astype(jnp.int32)
    boundary_mask = set_ends((jax.random.randint(arg_keys[7], (NX, NY, GZ), 0, 6) < 1).astype(jnp.int32), jax.random.fold_in(arg_keys[7], 1), 0, 1)
    leaving_block = draw_leaving_block(jax.random.fold_in(arg_keys[10], 71), 0)
    leaving_dest = draw_leaving_dest(jax.random.fold_in(arg_keys[10], 71), 0)
    return dict(position=position, velocity=velocity, affine=affine, deform=deform, particle_mass=particle_mass, block_count=block_count, block_brick=block_brick, boundary_mask=boundary_mask, leaving_block=leaving_block, leaving_dest=leaving_dest)


time_step = 0.05
shear_modulus = 8.0
lame_first = 12.0
stress_factor = 0.2
gravity = (2.0, 0.0, -9.0)
mass_floor = 1.0
highest = lax.Precision.HIGHEST
move_list = ((-1, -1), (-1, 0), (-1, 1), (0, -1), (0, 1), (1, -1), (1, 0), (1, 1))


def spline(distance):
    magnitude = jnp.abs(distance)
    inner_part = 0.75 - magnitude * magnitude
    outer_part = 0.5 * jnp.square(jnp.maximum(1.5 - magnitude, 0.0))
    return jnp.where(magnitude < 0.5, inner_part, outer_part)


def node_offsets():
    along_x = jnp.arange(2 * BX, dtype=jnp.float32)
    along_y = jnp.arange(2 * BY, dtype=jnp.float32)
    along_z = jnp.arange(2 * BZ, dtype=jnp.float32)
    node_shape = (2 * BX, 2 * BY, 2, BZ)
    halves = jnp.arange(2, dtype=jnp.float32)
    cells = jnp.arange(BZ, dtype=jnp.float32)
    height = halves[:, None] * BZ + cells[None, :]
    coords = jnp.stack([
        jnp.broadcast_to(along_x[:, None, None, None], node_shape).reshape(-1, BZ),
        jnp.broadcast_to(along_y[None, :, None, None], node_shape).reshape(-1, BZ),
        jnp.broadcast_to(height[None, None, :, :], node_shape).reshape(-1, BZ)])
    return along_x, along_y, along_z, coords


def spline_weights(position):
    along_x, along_y, along_z, coords = node_offsets()
    weight_x = spline(position[0][None] - along_x[:, None, None])
    weight_y = spline(position[1][None] - along_y[:, None, None])
    weight_z = spline(position[2][None] - along_z[:, None, None])
    joined = weight_x[:, None, None] * weight_y[None, :, None] * weight_z[None, None, :]
    return joined.reshape(-1, BZ, joined.shape[3], joined.shape[4]), coords


def brick_index(block_brick):
    cells = jnp.arange(BZ, dtype=jnp.int32)
    return (block_brick[None, :] * BZ + cells[:, None]).astype(jnp.int32)


def matrix_entry(matrix, row_index, column):
    return matrix[3 * row_index + column]


def particle_terms(position, velocity, affine, deform, weighed):
    determinant = (matrix_entry(deform, 0, 0) * (matrix_entry(deform, 1, 1) * matrix_entry(deform, 2, 2) - matrix_entry(deform, 1, 2) * matrix_entry(deform, 2, 1))
                   - matrix_entry(deform, 0, 1) * (matrix_entry(deform, 1, 0) * matrix_entry(deform, 2, 2) - matrix_entry(deform, 1, 2) * matrix_entry(deform, 2, 0))
                   + matrix_entry(deform, 0, 2) * (matrix_entry(deform, 1, 0) * matrix_entry(deform, 2, 1) - matrix_entry(deform, 1, 1) * matrix_entry(deform, 2, 0)))
    log_volume = jnp.log(determinant)
    momentum_matrix = []
    for row_index in range(3):
        for column in range(3):
            product = sum(matrix_entry(deform, row_index, inner_axis) * matrix_entry(deform, column, inner_axis) for inner_axis in range(3))
            identity = 1.0 if row_index == column else 0.0
            kirchhoff = shear_modulus * (product - identity) + lame_first * log_volume * identity
            momentum_matrix.append(weighed * (matrix_entry(affine, row_index, column) - stress_factor * kirchhoff))
    carried = [weighed * velocity[row_index] - sum(momentum_matrix[3 * row_index + inner_axis] * position[inner_axis] for inner_axis in range(3)) for row_index in range(3)]
    return jnp.stack([weighed] + carried + momentum_matrix, axis=0)


def block_grids(weights, quantities, coords):
    block_totals = jnp.einsum("kbp,gcbp->kgcb", quantities, weights, precision=highest)
    momentum_rows = [block_totals[1 + row_index] + sum(block_totals[4 + 3 * row_index + inner_axis] * coords[inner_axis][:, :, None] for inner_axis in range(3)) for row_index in range(3)]
    return jnp.stack([block_totals[0]] + momentum_rows, axis=0)


def bricks_to_grid(table, components):
    shaped = table.reshape(components, 2, BX, 2, BY, 2, NBX, NBY, GZ)
    total_grid = jnp.zeros((components, GX + BX, GY + BY, GZ + BZ), jnp.float32)
    for shift_x in (0, 1):
        for shift_y in (0, 1):
            for shift_z in (0, 1):
                brick_piece = shaped[:, shift_x, :, shift_y, :, shift_z]
                brick_piece = jnp.transpose(brick_piece, (0, 3, 1, 4, 2, 5)).reshape(components, GX, GY, GZ)
                total_grid = total_grid + jnp.pad(brick_piece, ((0, 0), (shift_x * BX, (1 - shift_x) * BX), (shift_y * BY, (1 - shift_y) * BY), (shift_z * BZ, (1 - shift_z) * BZ)))
    return total_grid


def grid_to_bricks(padded, components):
    pieces_x = []
    for shift_x in (0, 1):
        pieces_y = []
        for shift_y in (0, 1):
            pieces_z = []
            for shift_z in (0, 1):
                window = padded[:, shift_x * BX:shift_x * BX + GX, shift_y * BY:shift_y * BY + GY, shift_z * BZ:shift_z * BZ + GZ]
                window = window.reshape(components, NBX, BX, NBY, BY, GZ)
                pieces_z.append(jnp.transpose(window, (0, 2, 4, 1, 3, 5)))
            pieces_y.append(jnp.stack(pieces_z, axis=3))
        pieces_x.append(jnp.stack(pieces_y, axis=2))
    stacked = jnp.stack(pieces_x, axis=1)
    return stacked.reshape(components * 8 * BX * BY, NBX * NBY * GZ)


def live_mass(particle_mass, block_count):
    slot_index = lax.broadcasted_iota(jnp.int32, particle_mass.shape, 1)
    live_slots = (slot_index < block_count[:, None]).astype(jnp.float32)
    return live_slots, particle_mass * live_slots


def scatter_particles(position, velocity, affine, deform, particle_mass, block_count, block_brick):
    live_slots, weighed = live_mass(particle_mass, block_count)
    weights, coords = spline_weights(position)
    quantities = particle_terms(position, velocity, affine, deform, weighed)
    per_block = block_grids(weights, quantities, coords)
    flat = per_block.reshape(-1, BZ, per_block.shape[3])
    table = jnp.zeros((flat.shape[0], NBX * NBY * GZ), jnp.float32).at[:, brick_index(block_brick)].add(flat)
    return bricks_to_grid(table, 4), weights, coords, live_slots, weighed


def node_velocity(summed, boundary_mask):
    movable = (1 - boundary_mask).astype(jnp.float32)
    divisor = jnp.maximum(summed[0], mass_floor)
    return jnp.stack([movable * (summed[1 + axis_index] / divisor + time_step * gravity[axis_index]) for axis_index in range(3)])


def gather_particles(weights, coords, brick_velocity, position, deform, live_slots):
    rows_list = [brick_velocity[row_index] for row_index in range(3)]
    rows_list = rows_list + [brick_velocity[row_index] * coords[column][:, :, None] for row_index in range(3) for column in range(3)]
    node_table = jnp.stack(rows_list, axis=0)
    result = jnp.einsum("gcbp,kgcb->kbp", weights, node_table, precision=highest)
    new_velocity = [result[row_index] for row_index in range(3)]
    new_affine = [4.0 * (result[3 + 3 * row_index + column] - new_velocity[row_index] * position[column]) for row_index in range(3) for column in range(3)]
    new_deform = []
    for row_index in range(3):
        for column in range(3):
            advanced = deform[3 * row_index + column] + time_step * sum(new_affine[3 * row_index + inner_axis] * deform[3 * inner_axis + column] for inner_axis in range(3))
            new_deform.append(advanced)
    new_position = [position[row_index] + time_step * new_velocity[row_index] for row_index in range(3)]
    return jnp.stack(new_position + new_velocity + new_affine + new_deform) * live_slots


def fetch_bricks(padded, block_brick):
    table = grid_to_bricks(padded, 3)
    fetched = jnp.take(table, brick_index(block_brick), axis=1)
    return fetched.reshape(3, -1, BZ, block_brick.shape[0])


def outgoing_blocks(carried_state, leaving_block, leaving_dest):
    labels = jnp.arange(9, dtype=jnp.int32)
    onehot = (leaving_dest[:, None] == labels[None, :]).astype(jnp.int32)
    earlier = jnp.cumsum(onehot, axis=0) - onehot
    entry_rank = jnp.sum(earlier * onehot, axis=1)
    slot_index = jnp.arange(8 * MIG, dtype=jnp.int32)
    move_index = slot_index // MIG
    wanted = move_index + (move_index >= 4).astype(jnp.int32)
    matches = (leaving_dest[None, :] == wanted[:, None]) & (entry_rank[None, :] == (slot_index % MIG)[:, None])
    source = jnp.sum(matches.astype(jnp.int32) * leaving_block[None, :], axis=1)
    present = jnp.any(matches, axis=1).astype(jnp.float32)
    return jnp.take(carried_state, source, axis=1) * present[None, :, None]


def staying_blocks(leaving_block, leaving_dest, blocks):
    hit_table = (leaving_block[:, None] == jnp.arange(blocks, dtype=jnp.int32)[None, :]) & (leaving_dest[:, None] != 4)
    return 1.0 - jnp.any(hit_table, axis=0).astype(jnp.float32)


def reference(position, velocity, affine, deform, particle_mass, block_count, block_brick, boundary_mask, leaving_block, leaving_dest):
    devices = N_DOWN * N_CROSS

    def split_rows(mesh_array):
        return jnp.moveaxis(mesh_array.reshape(mesh_array.shape[0], devices, BLOCKS, SLOTS), 1, 0)

    stacks = (split_rows(position), split_rows(velocity), split_rows(affine), split_rows(deform),
              particle_mass.reshape(devices, BLOCKS, SLOTS), block_count.reshape(devices, BLOCKS),
              block_brick.reshape(devices, BLOCKS))

    def scatter_one(inputs):
        return scatter_particles(*inputs)[0]

    local_grids = lax.map(scatter_one, stacks)
    shape_local = (4, GX + BX, GY + BY, GZ + BZ)

    def corner_start(device):
        device = device.astype(jnp.int32)
        return (jnp.int32(0), (device // N_CROSS) * GX, (device % N_CROSS) * GY, jnp.int32(0))

    def place_grid(device, total_grid):
        region = lax.dynamic_slice(total_grid, corner_start(device), shape_local)
        return lax.dynamic_update_slice(total_grid, region + local_grids[device], corner_start(device))

    total_grid = lax.fori_loop(0, devices, place_grid, jnp.zeros((4, NX + BX, NY + BY, GZ + BZ), jnp.float32))
    node_field = node_velocity(total_grid[:, :NX, :NY, :GZ], boundary_mask)
    padded = jnp.pad(node_field, ((0, 0), (0, BX), (0, BY), (0, BZ)))

    def gather_one(inputs):
        device = inputs[0]
        window = lax.dynamic_slice(padded, corner_start(device), (3, GX + BX, GY + BY, GZ + BZ))
        live_slots, weighed = live_mass(inputs[5], inputs[6])
        weights, coords = spline_weights(inputs[1])
        brick_velocity = fetch_bricks(window, inputs[7])
        updated = gather_particles(weights, coords, brick_velocity, inputs[1], inputs[4], live_slots)
        staying = staying_blocks(inputs[8], inputs[9], BLOCKS)
        carried_state = jnp.concatenate([updated, weighed[None]], axis=0)
        outgoing = outgoing_blocks(carried_state, inputs[8], inputs[9])
        return updated * staying[None, :, None], outgoing

    device_ids = jnp.arange(devices, dtype=jnp.int32)
    states, outgoing = lax.map(gather_one, (device_ids,) + stacks + (leaving_block.reshape(devices, LIST), leaving_dest.reshape(devices, LIST)))
    new_state = jnp.moveaxis(states, 0, 1).reshape(24, devices * BLOCKS, SLOTS)
    grouped = outgoing.reshape(N_DOWN, N_CROSS, 25, 8, MIG, SLOTS)

    def displace(mesh_array, step_down, step_cross):
        padded_mesh = jnp.pad(mesh_array, ((1, 1), (1, 1)) + ((0, 0),) * (mesh_array.ndim - 2))
        return padded_mesh[1 - step_down:1 - step_down + N_DOWN, 1 - step_cross:1 - step_cross + N_CROSS]

    arrived = [displace(grouped[:, :, :, move_index], move[0], move[1]) for move_index, move in enumerate(move_list)]
    arrivals = jnp.stack(arrived, axis=3)
    arrivals = jnp.moveaxis(arrivals, 2, 0).reshape(25, devices * 8 * MIG, SLOTS)
    return new_state, arrivals
```

```python
import functools

import jax
import jax.numpy as jnp
from jax import lax
from jax.experimental import pallas as pl
from jax.experimental.pallas import tpu as pltpu
from jax.sharding import PartitionSpec as P

GX = 16
GY = 16
GZ = 128
SLOTS = 128
BLOCKS = 64
MIG = 8
NBX = 8
NBY = 8

time_step = 0.05
shear_modulus = 8.0
lame_first = 12.0
stress_factor = 0.2
gravity = (2.0, 0.0, -9.0)
mass_floor = 1.0
move_list = ((-1, -1), (-1, 0), (-1, 1), (0, -1), (0, 1), (1, -1), (1, 0), (1, 1))
early_order = (0, 2, 5, 7, 3, 4, 1, 6)
early_first = 4

MESH = pl.DeviceIdType.MESH
f32 = jnp.float32
bf16 = jnp.bfloat16


def spline(distance):
    magnitude = jnp.abs(distance)
    outer_part = jnp.maximum(1.5 - magnitude, 0.0)
    return jnp.where(magnitude < 0.5, 0.75 - magnitude * magnitude, 0.5 * outer_part * outer_part)


def row_iota(rows):
    return lax.broadcasted_iota(jnp.int32, (rows, 128), 0)


def lane_iota(rows):
    return lax.broadcasted_iota(jnp.int32, (rows, 128), 1)


def plane_weights(x0, x1):
    parity = (row_iota(8) & 1).astype(f32)
    dx = [float(x) - x0 for x in range(4)]
    wx = [spline(d) for d in dx]
    dy = [(parity + 2.0 * yp) - x1 for yp in range(2)]
    wy = [spline(d) for d in dy]
    return dx, wx, dy, wy


def split(value):
    high = value.astype(bf16)
    low = (value - high.astype(f32)).astype(bf16)
    return high, low


def particle_rows(deform, affine, velocity, mass):
    d = deform
    determinant = (
        d[0] * (d[4] * d[8] - d[5] * d[7])
        - d[1] * (d[3] * d[8] - d[5] * d[6])
        + d[2] * (d[3] * d[7] - d[4] * d[6])
    )
    pressure = lame_first * jnp.log(determinant)
    columns = [[None] * 3 for _ in range(3)]
    for a in range(3):
        for c in range(a, 3):
            product = d[3 * a] * d[3 * c] + d[3 * a + 1] * d[3 * c + 1] + d[3 * a + 2] * d[3 * c + 2]
            if a == c:
                tau = shear_modulus * (product - 1.0) + pressure
            else:
                tau = shear_modulus * product
            columns[c][a] = mass * (affine[3 * a + c] - stress_factor * tau)
            if a != c:
                columns[a][c] = mass * (affine[3 * c + a] - stress_factor * tau)
    return [mass] + [mass * v for v in velocity], columns


def gathered(lhs_f32, x0, x1, x2, limit):
    lane = lane_iota(64)
    high = lhs_f32.astype(bf16).astype(f32)
    low = lhs_f32 - high
    lhs = jnp.where((lane >= 8) & (lane < 16), low, high)
    lhs = jnp.where(lane < 24, lhs, 0.0).astype(bf16)
    height = row_iota(8)
    dz = height.astype(f32) - x2
    wz = spline(dz)
    if limit is not None:
        wz = jnp.where(height < limit, wz, 0.0)
    rhs = jnp.concatenate([wz, wz * dz], axis=1)
    rhs_high = rhs.astype(bf16).astype(f32)
    rhs_low = rhs - rhs_high
    stacked = jnp.concatenate([rhs_high, rhs_high, rhs_low, jnp.zeros_like(rhs)], axis=0).astype(bf16)
    u = jnp.dot(lhs[:, :32], stacked, preferred_element_type=f32)
    dx, wx, dy, wy = plane_weights(x0, x1)
    wyd = [w * d for w, d in zip(wy, dy)]
    total = None
    for x in range(4):
        a = b = c = None
        for yp in range(2):
            start = 8 * (2 * x + yp)
            u0 = u[start : start + 8, :128]
            u1 = u[start : start + 8, 128:]
            terms = (wy[yp] * u0, wyd[yp] * u0, wy[yp] * u1)
            a, b, c = terms if a is None else (a + terms[0], b + terms[1], c + terms[2])
        parts = (wx[x] * a, (wx[x] * dx[x]) * a, wx[x] * b, wx[x] * c)
        total = parts if total is None else tuple(t + p for t, p in zip(total, parts))
    return total


def final_rows(sums_ref, base, position, deform):
    def both(row):
        return sums_ref[pl.ds(base + row, 8, stride=32), :] + sums_ref[pl.ds(base + row + 1, 8, stride=32), :]

    v = [both(2 + 2 * a) for a in range(3)]
    c = [4.0 * both(8 * (1 + col) + 2 + 2 * a) for a in range(3) for col in range(3)]
    x = [position[a] + time_step * v[a] for a in range(3)]
    f = []
    for a in range(3):
        for col in range(3):
            grown = c[3 * a] * deform[col] + c[3 * a + 1] * deform[3 + col] + c[3 * a + 2] * deform[6 + col]
            f.append(deform[3 * a + col] + time_step * grown)
    return x + v + c + f


def kernel(
    n_down,
    n_cross,
    next_ref,
    first_ref,
    column_ref,
    lift_ref,
    source_ref,
    pos_ref,
    vel_ref,
    aff_ref,
    def_ref,
    mass_ref,
    present_ref,
    stay_ref,
    mask_ref,
    state_ref,
    arrive_ref,
    early,
    early_in,
    late,
    late_in,
    table,
    chain,
    grid,
    node_v,
    movable,
    mask_y,
    mask_x_in,
    mask_y_in,
    mask_c_in,
    face_x,
    face_y,
    corner,
    sums,
    early_send,
    early_recv,
    late_send,
    late_recv,
    halo_send,
    halo_recv,
    mask_send,
    mask_recv,
):
    i = lax.axis_index("down")
    j = lax.axis_index("cross")

    def device(a, b):
        return (lax.rem(i + (a + n_down), n_down), lax.rem(j + (b + n_cross), n_cross))

    def inside(a, b):
        valid = None
        if a:
            valid = (i + a >= 0) & (i + a < n_down)
        if b:
            other = (j + b >= 0) & (j + b < n_cross)
            valid = other if valid is None else valid & other
        return valid.astype(f32)

    barrier = pltpu.get_barrier_semaphore()
    for a, b in move_list:
        pl.semaphore_signal(barrier, inc=1, device_id=device(a, b), device_id_type=MESH)

    for move in range(8):

        def pick(k, carry, move=move):
            source = source_ref[move * 8 + k]
            early[move, 0:3, pl.ds(k, 1), :] = pos_ref[:, pl.ds(source, 1), :]
            early[move, 3:12, pl.ds(k, 1), :] = def_ref[:, pl.ds(source, 1), :]
            early[move, 12, pl.ds(k, 1), :] = (
                mass_ref[pl.ds(source, 1), :] * present_ref[pl.ds(move * 8 + k, 1), :]
            )
            return carry

        lax.fori_loop(0, 8, pick, 0)
    for par in range(2):
        mask_y[par] = mask_ref[pl.ds(par, 16, stride=16), :]

    def remote(source, target, send, recv, a, b):
        return pltpu.make_async_remote_copy(
            src_ref=source,
            dst_ref=target,
            send_sem=send,
            recv_sem=recv,
            device_id=device(a, b),
            device_id_type=MESH,
        )

    early_copies = [
        remote(early.at[m], early_in.at[m], early_send.at[m], early_recv.at[m], a, b)
        for m, (a, b) in enumerate(move_list)
    ]
    late_copies = [
        remote(late.at[m], late_in.at[m], late_send.at[m], late_recv.at[m], a, b)
        for m, (a, b) in enumerate(move_list)
    ]
    mask_copies = [
        remote(mask_y, mask_y_in, mask_send.at[0], mask_recv.at[0], 0, -1),
        remote(mask_ref.at[pl.ds(0, 32)], mask_x_in, mask_send.at[1], mask_recv.at[1], -1, 0),
        remote(mask_y.at[:, pl.ds(0, 8)], mask_c_in, mask_send.at[2], mask_recv.at[2], -1, -1),
    ]

    pl.semaphore_wait(barrier, 8)
    for copy in mask_copies:
        copy.start()
    for m in early_order[:early_first]:
        early_copies[m].start()

    def terms(g, carry):
        rows = pl.ds(pl.multiple_of(g * 8, 8), 8)
        deform = [def_ref[c, rows, :] for c in range(9)]
        affine = [aff_ref[c, rows, :] for c in range(9)]
        velocity = [vel_ref[c, rows, :] for c in range(3)]
        moved, columns = particle_rows(deform, affine, velocity, mass_ref[rows, :])
        zero = jnp.zeros((8, 128), f32)
        lists = [moved] + [[zero] + columns[c] for c in range(3)]
        for group, values in enumerate(lists):
            for quantity, value in enumerate(values):
                for par in range(2):
                    row = g * 256 + (8 * group + 2 * quantity + par)
                    table[pl.ds(row, 8, stride=32), :] = value
        return carry

    lax.fori_loop(0, 8, terms, 0)

    chain[BLOCKS] = jnp.zeros((64, 128), f32)

    def to_bricks(step, carry):
        b = (BLOCKS - 1) - step
        lift = lift_ref[b]
        x0 = pos_ref[0, pl.ds(b, 1), :]
        x1 = pos_ref[1, pl.ds(b, 1), :]
        x2 = pos_ref[2, pl.ds(b, 1), :]
        base = pl.multiple_of(b * 32, 32)
        moved = table[pl.ds(base, 8), :]
        col0 = table[pl.ds(base + 8, 8), :]
        col1 = table[pl.ds(base + 16, 8), :]
        col2 = table[pl.ds(base + 24, 8), :]
        dx, wx, dy, wy = plane_weights(x0, x1)
        plain, raised = [], []
        for x in range(4):
            at_x = moved + col0 * dx[x]
            for yp in range(2):
                weight = wx[x] * wy[yp]
                plain.append((at_x + col1 * dy[yp]) * weight)
                raised.append(col2 * weight)
        lhs = jnp.concatenate([jnp.concatenate(plain, axis=0), jnp.concatenate(raised, axis=0)], axis=1)
        lhs_high, lhs_low = split(lhs)
        height = row_iota(8)
        dz = height.astype(f32) - x2
        wz = jnp.where(height + lift < GZ, spline(dz), 0.0)
        rhs = jnp.concatenate([wz, wz * dz], axis=1)
        rhs_high = rhs.astype(bf16).astype(f32)
        stacked = jnp.concatenate([rhs_high, rhs - rhs_high], axis=0).astype(bf16)
        contract = (((1,), (1,)), ((), ()))
        found = lax.dot_general(lhs_high, stacked, contract, preferred_element_type=f32)
        found = found + lax.dot_general(lhs_low, stacked, contract, preferred_element_type=f32)
        wide = jnp.concatenate([found, jnp.zeros((64, 112), f32)], axis=1)
        folded = pltpu.roll(wide, lift, 1) + pltpu.roll(wide, (lift + 120) & 127, 1)
        lane = lane_iota(64)
        here = (lane >= lift) & (lane < lift + 8)
        chain[b] = jnp.where(here, folded, 0.0) + chain[next_ref[b]]
        return carry

    lax.fori_loop(0, BLOCKS, to_bricks, 0)

    def clear(x, carry):
        grid[x] = jnp.zeros((9, 8, 128), f32)
        return carry

    lax.fori_loop(0, 18, clear, 0)

    def spread(column, carry):
        p = column // NBY
        q = lax.rem(column, NBY)
        first = first_ref[column]
        for x in range(4):
            for yp in range(2):
                start = 8 * (2 * x + yp)
                grid[2 * p + x, q + yp] += chain[first, start : start + 8, :]
        return carry

    lax.fori_loop(0, NBX * NBY, spread, 0)

    halo_copies = []
    faces = {-1: 0, 1: 1}
    for m, (a, b) in enumerate(move_list):
        xs = pl.ds(16, 2) if a == 1 else pl.ds(0, 2)
        y = 8 if b == 1 else 0
        if b == 0:
            source, target = grid.at[xs], face_x.at[faces[a]]
        elif a == 0:
            source, target = grid.at[:, y], face_y.at[faces[b]]
        else:
            source, target = grid.at[xs, y], corner.at[2 * faces[a] + faces[b]]
        halo_copies.append(remote(source, target, halo_send.at[m], halo_recv.at[m], a, b))
    for m in (3, 4, 0, 2, 5, 7, 1, 6):
        halo_copies[m].start()
    for m in early_order[early_first:]:
        early_copies[m].start()

    def own_mask(x, carry):
        movable[x, 0:16, :] = (1 - mask_ref[pl.ds(pl.multiple_of(x * 16, 16), 16), :]).astype(f32)
        return carry

    lax.fori_loop(0, 16, own_mask, 0)
    row8 = row_iota(8)
    even = (row8 & 1) == 0
    quantity = row8 // 2
    pull = jnp.where(quantity == 1, time_step * gravity[0], 0.0)
    pull = jnp.where(quantity == 2, time_step * gravity[1], pull)
    pull = jnp.where(quantity == 3, time_step * gravity[2], pull)

    def put_velocity(x, yp, tile):
        mass = jnp.where(row8 < 2, tile, 0.0)
        mass = mass + pltpu.roll(mass, 2, 0)
        mass = mass + pltpu.roll(mass, 4, 0)
        free = jnp.where(even, movable[x, pl.ds(2 * yp, 1), :], movable[x, pl.ds(2 * yp + 1, 1), :])
        node_v[x, yp] = free * (tile / jnp.maximum(mass, mass_floor) + pull)

    def interior(x, carry):
        for yp in range(1, 8):
            put_velocity(x, yp, grid[x, yp])
        return carry

    lax.fori_loop(2, 16, interior, 0)
    for copy in mask_copies:
        copy.wait()
    past_x = inside(1, 0)
    past_y = inside(0, 1)
    past_c = inside(1, 1)
    for xx in range(2):
        movable[16 + xx, 0:16, :] = (1 - mask_x_in[pl.ds(16 * xx, 16), :]).astype(f32) * past_x
        for par in range(2):
            movable[16 + xx, 16 + par : 17 + par, :] = (
                1 - mask_c_in[par, xx : xx + 1, :]
            ).astype(f32) * past_c

    def side_mask(x, carry):
        for par in range(2):
            movable[x, 16 + par : 17 + par, :] = (1 - mask_y_in[par, pl.ds(x, 1), :]).astype(f32) * past_y
        return carry

    lax.fori_loop(0, 16, side_mask, 0)
    for copy in halo_copies:
        copy.wait()
    has = {(a, b): inside(-a, -b) for a, b in move_list}

    def low_high(yp):
        for a in (-1, 1):
            for xx in range(2):
                x = xx if a == 1 else 16 + xx
                yield a, xx, x, grid[x, yp] + face_x[faces[a], xx, yp] * has[(a, 0)]

    def edge_x(yp, carry):
        for _, _, x, tile in low_high(yp):
            put_velocity(x, yp, tile)
        return carry

    lax.fori_loop(1, 8, edge_x, 0)

    def edge_y(x, carry):
        for b in (-1, 1):
            yp = 0 if b == 1 else 8
            put_velocity(x, yp, grid[x, yp] + face_y[faces[b], x] * has[(0, b)])
        return carry

    lax.fori_loop(2, 16, edge_y, 0)
    for b in (-1, 1):
        yp = 0 if b == 1 else 8
        for a, xx, x, tile in low_high(yp):
            tile = tile + face_y[faces[b], x] * has[(0, b)]
            tile = tile + corner[2 * faces[a] + faces[b], xx] * has[(a, b)]
            put_velocity(x, yp, tile)

    lane8 = lane_iota(8)

    def brick_tiles(b):
        column = column_ref[b]
        p = column // NBY
        q = lax.rem(column, NBY)
        return [node_v[2 * p + x, q + yp] for x in range(4) for yp in range(2)]

    for move in range(8):

        def window(k, carry, move=move):
            b = source_ref[move * 8 + k]
            lift = lift_ref[b]
            tiles = brick_tiles(b)
            shift = (8 * k - lift + 128) & 127
            local = lane8 - 8 * k
            low = (local >= 0) & (local < 8) & (local + lift < GZ)
            local = local - 64
            high = (local >= 0) & (local < 8) & (local + lift < GZ)
            out = []
            for t in range(4):
                kept = jnp.where(low, pltpu.roll(tiles[t], shift, 1), carry[t])
                out.append(jnp.where(high, pltpu.roll(tiles[t + 4], (shift + 64) & 127, 1), kept))
            return tuple(out)

        zero = jnp.zeros((8, 128), f32)
        packed = lax.fori_loop(0, 8, window, (zero,) * 4)
        for t in range(3):
            moved = pltpu.roll(packed[3], (8 - (2 + 2 * t)) & 7, 0)
            late[move, t] = jnp.where(row8 < 2, moved, packed[t])
        late_copies[move].start()

    lane64 = lane_iota(64)

    def windows(stack, shift):
        first = pltpu.roll(stack, shift & 127, 1)
        second = pltpu.roll(stack, (shift + 8) & 127, 1)
        third = pltpu.roll(stack, (shift + 16) & 127, 1)
        return jnp.where(lane64 < 8, first, jnp.where(lane64 < 16, second, third))

    def put_sums(b, total):
        base = pl.multiple_of(b * 32, 32)
        for t in range(4):
            sums[pl.ds(base + 8 * t, 8), :] = total[t]

    def resident(b, carry):
        lift = lift_ref[b]
        stack = jnp.concatenate(brick_tiles(b), axis=0)
        total = gathered(
            windows(stack, 128 - lift),
            pos_ref[0, pl.ds(b, 1), :],
            pos_ref[1, pl.ds(b, 1), :],
            pos_ref[2, pl.ds(b, 1), :],
            GZ - lift,
        )
        put_sums(b, total)
        return carry

    lax.fori_loop(0, BLOCKS, resident, 0)

    def finish(g, carry):
        rows = pl.ds(pl.multiple_of(g * 8, 8), 8)
        position = [pos_ref[c, rows, :] for c in range(3)]
        deform = [def_ref[c, rows, :] for c in range(9)]
        keep = jnp.where(mass_ref[rows, :] > 0.0, stay_ref[rows, :], 0.0)
        for row, value in enumerate(final_rows(sums, g * 256, position, deform)):
            state_ref[row, rows, :] = value * keep
        return carry

    lax.fori_loop(0, 8, finish, 0)

    for move, (a, b) in enumerate(move_list):
        early_copies[move].wait()
        late_copies[move].wait()
        packed = [late_in[move, t] for t in range(3)]
        last = jnp.zeros((8, 128), f32)
        for t in range(3):
            last = last + pltpu.roll(jnp.where(row8 < 2, packed[t], 0.0), 2 + 2 * t, 0)
        packed.append(last)
        low_stack = jnp.concatenate(packed, axis=0)
        stack = jnp.concatenate([low_stack, pltpu.roll(low_stack, 64, 1)], axis=0)

        def arriving(k, carry, move=move, stack=stack):
            total = gathered(
                windows(stack, 128 - 8 * k),
                early_in[move, 0, pl.ds(k, 1), :],
                early_in[move, 1, pl.ds(k, 1), :],
                early_in[move, 2, pl.ds(k, 1), :],
                None,
            )
            put_sums(k, total)
            return carry

        lax.fori_loop(0, 8, arriving, 0)
        rows = pl.ds(move * 8, 8)
        position = [early_in[move, c] for c in range(3)]
        deform = [early_in[move, 3 + c] for c in range(9)]
        mass = early_in[move, 12] * inside(-a, -b)
        keep = jnp.where(mass > 0.0, 1.0, 0.0)
        for row, value in enumerate(final_rows(sums, 0, position, deform)):
            arrive_ref[row, rows, :] = value * keep
        arrive_ref[24, rows, :] = mass


def brick_tables(block_brick):
    column = block_brick // 32
    ids = jnp.arange(BLOCKS, dtype=jnp.int32)
    later = (column[:, None] == column[None, :]) & (ids[None, :] > ids[:, None])
    following = jnp.min(jnp.where(later, ids[None, :], BLOCKS), axis=1)
    held = column[None, :] == jnp.arange(NBX * NBY, dtype=jnp.int32)[:, None]
    first = jnp.min(jnp.where(held, ids[None, :], BLOCKS), axis=1)
    return following, first, column, (block_brick % 32) * 4


def leaving_tables(leaving_block, leaving_dest):
    order = jnp.arange(BLOCKS, dtype=jnp.int32)
    ahead = (leaving_dest[:, None] == leaving_dest[None, :]) & (order[None, :] < order[:, None])
    entry_rank = jnp.sum(ahead.astype(jnp.int32), axis=1)
    slot_index = jnp.arange(8 * MIG, dtype=jnp.int32)
    move_index = slot_index // MIG
    wanted = move_index + (move_index >= 4).astype(jnp.int32)
    matches = (leaving_dest[None, :] == wanted[:, None]) & (entry_rank[None, :] == (slot_index % MIG)[:, None])
    source = jnp.sum(matches.astype(jnp.int32) * leaving_block[None, :], axis=1)
    present = jnp.any(matches, axis=1).astype(f32)
    hit_table = (leaving_block[:, None] == order[None, :]) & (leaving_dest[:, None] != 4)
    staying = 1.0 - jnp.any(hit_table, axis=0).astype(f32)
    return source, present, staying


def body(
    n_down,
    n_cross,
    position,
    velocity,
    affine,
    deform,
    particle_mass,
    block_count,
    block_brick,
    boundary_mask,
    leaving_block,
    leaving_dest,
):
    slot_index = lax.broadcasted_iota(jnp.int32, particle_mass.shape, 1)
    weighed = jnp.where(slot_index < block_count[:, None], particle_mass, 0.0)
    following, first, column, lift = brick_tables(block_brick)
    source, present, staying = leaving_tables(leaving_block, leaving_dest)
    wide = (BLOCKS, SLOTS)
    present = jnp.broadcast_to(present[:, None], wide)
    staying = jnp.broadcast_to(staying[:, None], wide)
    smem = pl.BlockSpec(memory_space=pltpu.SMEM)
    vmem = pl.BlockSpec(memory_space=pltpu.VMEM)
    dma = pltpu.SemaphoreType.DMA
    return pl.pallas_call(
        functools.partial(kernel, n_down, n_cross),
        out_shape=(
            jax.ShapeDtypeStruct((24, BLOCKS, SLOTS), f32),
            jax.ShapeDtypeStruct((25, BLOCKS, SLOTS), f32),
        ),
        in_specs=[smem] * 5 + [vmem] * 8,
        out_specs=(vmem, vmem),
        scratch_shapes=[
            pltpu.VMEM((8, 13, 8, 128), f32),
            pltpu.VMEM((8, 13, 8, 128), f32),
            pltpu.VMEM((8, 3, 8, 128), f32),
            pltpu.VMEM((8, 3, 8, 128), f32),
            pltpu.VMEM((BLOCKS * 32, 128), f32),
            pltpu.VMEM((BLOCKS + 1, 64, 128), f32),
            pltpu.VMEM((18, 9, 8, 128), f32),
            pltpu.VMEM((18, 9, 8, 128), f32),
            pltpu.VMEM((18, 24, 128), f32),
            pltpu.VMEM((2, 16, 128), jnp.int32),
            pltpu.VMEM((32, 128), jnp.int32),
            pltpu.VMEM((2, 16, 128), jnp.int32),
            pltpu.VMEM((2, 8, 128), jnp.int32),
            pltpu.VMEM((2, 2, 9, 8, 128), f32),
            pltpu.VMEM((2, 18, 8, 128), f32),
            pltpu.VMEM((4, 2, 8, 128), f32),
            pltpu.VMEM((BLOCKS * 32, 128), f32),
            dma((8,)),
            dma((8,)),
            dma((8,)),
            dma((8,)),
            dma((8,)),
            dma((8,)),
            dma((3,)),
            dma((3,)),
        ],
        compiler_params=pltpu.CompilerParams(collective_id=0, has_side_effects=True),
    )(
        following,
        first,
        column,
        lift,
        source,
        position,
        velocity,
        affine,
        deform,
        weighed,
        present,
        staying,
        boundary_mask.reshape(GX * GY, GZ),
    )


def solution(mesh):
    blocks = P(None, ("down", "cross"), None)
    flat = P(("down", "cross"))
    in_specs = (
        blocks,
        blocks,
        blocks,
        blocks,
        P(("down", "cross"), None),
        flat,
        flat,
        P("down", "cross", None),
        flat,
        flat,
    )
    step = functools.partial(body, mesh.shape["down"], mesh.shape["cross"])
    return jax.shard_map(step, mesh=mesh, in_specs=in_specs, out_specs=(blocks, blocks), check_vma=False)
```

```python
import functools

import jax
import jax.numpy as jnp
from jax import lax
from jax.experimental import pallas as pl
from jax.experimental.pallas import tpu as pltpu
from jax.sharding import PartitionSpec as P

GX = 16
GY = 16
GZ = 128
SLOTS = 128
BLOCKS = 64
MIG = 8
NBX = 8
NBY = 8

time_step = 0.05
shear_modulus = 8.0
lame_first = 12.0
stress_factor = 0.2
gravity = (2.0, 0.0, -9.0)
mass_floor = 1.0
move_list = ((-1, -1), (-1, 0), (-1, 1), (0, -1), (0, 1), (1, -1), (1, 0), (1, 1))
early_order = (0, 2, 5, 7, 3, 4, 1, 6)
early_first = 8
p2g_batch = 4
g2p_batch = 4

MESH = pl.DeviceIdType.MESH
f32 = jnp.float32
bf16 = jnp.bfloat16


def spline(distance):
    magnitude = jnp.abs(distance)
    outer_part = jnp.maximum(1.5 - magnitude, 0.0)
    return jnp.where(magnitude < 0.5, 0.75 - magnitude * magnitude, 0.5 * outer_part * outer_part)


def row_iota(rows):
    return lax.broadcasted_iota(jnp.int32, (rows, 128), 0)


def lane_iota(rows):
    return lax.broadcasted_iota(jnp.int32, (rows, 128), 1)


def plane_weights(x0, x1):
    parity = (row_iota(8) & 1).astype(f32)
    dx = [float(x) - x0 for x in range(4)]
    wx = [spline(d) for d in dx]
    dy = [(parity + 2.0 * yp) - x1 for yp in range(2)]
    wy = [spline(d) for d in dy]
    return dx, wx, dy, wy


def split(value):
    high = value.astype(bf16)
    low = (value - high.astype(f32)).astype(bf16)
    return high, low


def particle_rows(deform, affine, velocity, mass):
    d = deform
    determinant = (
        d[0] * (d[4] * d[8] - d[5] * d[7])
        - d[1] * (d[3] * d[8] - d[5] * d[6])
        + d[2] * (d[3] * d[7] - d[4] * d[6])
    )
    pressure = lame_first * jnp.log(determinant)
    columns = [[None] * 3 for _ in range(3)]
    for a in range(3):
        for c in range(a, 3):
            product = d[3 * a] * d[3 * c] + d[3 * a + 1] * d[3 * c + 1] + d[3 * a + 2] * d[3 * c + 2]
            if a == c:
                tau = shear_modulus * (product - 1.0) + pressure
            else:
                tau = shear_modulus * product
            columns[c][a] = mass * (affine[3 * a + c] - stress_factor * tau)
            if a != c:
                columns[a][c] = mass * (affine[3 * c + a] - stress_factor * tau)
    return [mass] + [mass * v for v in velocity], columns


def gathered(lhs_f32, x0, x1, x2, limit):
    lane = lane_iota(64)
    high = lhs_f32.astype(bf16).astype(f32)
    low = lhs_f32 - high
    lhs = jnp.where((lane >= 8) & (lane < 16), low, high)
    lhs = jnp.where(lane < 24, lhs, 0.0).astype(bf16)
    height = row_iota(8)
    dz = height.astype(f32) - x2
    wz = spline(dz)
    if limit is not None:
        wz = jnp.where(height < limit, wz, 0.0)
    rhs = jnp.concatenate([wz, wz * dz], axis=1)
    rhs_high = rhs.astype(bf16).astype(f32)
    rhs_low = rhs - rhs_high
    stacked = jnp.concatenate([rhs_high, rhs_high, rhs_low, jnp.zeros_like(rhs)], axis=0).astype(bf16)
    u = jnp.dot(lhs[:, :32], stacked, preferred_element_type=f32)
    dx, wx, dy, wy = plane_weights(x0, x1)
    wyd = [w * d for w, d in zip(wy, dy)]
    total = None
    for x in range(4):
        a = b = c = None
        for yp in range(2):
            start = 8 * (2 * x + yp)
            u0 = u[start : start + 8, :128]
            u1 = u[start : start + 8, 128:]
            terms = (wy[yp] * u0, wyd[yp] * u0, wy[yp] * u1)
            a, b, c = terms if a is None else (a + terms[0], b + terms[1], c + terms[2])
        parts = (wx[x] * a, (wx[x] * dx[x]) * a, wx[x] * b, wx[x] * c)
        total = parts if total is None else tuple(t + p for t, p in zip(total, parts))
    return total


def final_rows(sums_ref, base, position, deform):
    def both(row):
        return sums_ref[pl.ds(base + row, 8, stride=32), :] + sums_ref[pl.ds(base + row + 1, 8, stride=32), :]

    v = [both(2 + 2 * a) for a in range(3)]
    c = [4.0 * both(8 * (1 + col) + 2 + 2 * a) for a in range(3) for col in range(3)]
    x = [position[a] + time_step * v[a] for a in range(3)]
    f = []
    for a in range(3):
        for col in range(3):
            grown = c[3 * a] * deform[col] + c[3 * a + 1] * deform[3 + col] + c[3 * a + 2] * deform[6 + col]
            f.append(deform[3 * a + col] + time_step * grown)
    return x + v + c + f


def build_tables(count_ref, brick_ref, leave_ref, dest_ref, weight_ref, mass_ref, stay_ref, staged):
    shape = (128, 128)
    down = lax.broadcasted_iota(jnp.int32, shape, 0)
    across = lax.broadcasted_iota(jnp.int32, shape, 1)

    def padded(row, filler):
        return jnp.concatenate([row, jnp.full((1, 128 - BLOCKS), filler, jnp.int32)], axis=1)

    def upright(row):
        return jnp.transpose(jnp.broadcast_to(row, shape))

    def least(value):
        return jnp.min(value, axis=0, keepdims=True)

    count = upright(padded(count_ref[...], 0))[:BLOCKS]
    lane = across[:BLOCKS]
    mass_ref[...] = jnp.where(lane < count, weight_ref[...], 0.0)
    brick = padded(brick_ref[...], 0)
    column = brick >> 5
    sides = upright(column)[:BLOCKS]
    ids = down[:BLOCKS]
    staged[0:1, :] = least(jnp.where((sides == column) & (ids > lane), ids, BLOCKS))
    cell = ((sides >> 3) + 1) * 10 + (sides & 7) + 1
    staged[1:2, :] = least(jnp.where(cell == lane, ids, BLOCKS))
    staged[2:3, :] = column
    staged[3:4, :] = (brick & 31) * 4
    leave = padded(leave_ref[...], 0)
    dest = padded(dest_ref[...], 4)
    dest_up = upright(dest)[:BLOCKS]
    leave_up = upright(leave)[:BLOCKS]
    rank = jnp.sum(jnp.where((dest_up == dest) & (ids < lane), 1, 0), axis=0, keepdims=True)
    move = jnp.where(dest > 4, dest - 1, dest)
    slot = jnp.where(dest == 4, -1, move * 8 + rank)
    slot_up = upright(slot)[:BLOCKS]
    match = slot_up == lane
    staged[4:5, :] = jnp.sum(jnp.where(match, leave_up, 0), axis=0, keepdims=True)
    staged[5:6, :] = jnp.sum(jnp.where(match, 1, 0), axis=0, keepdims=True)
    staged[6:8, :] = jnp.zeros((2, 128), jnp.int32)
    gone = jnp.where((leave == ids) & (dest != 4), 1.0, 0.0)
    stay_ref[...] = jnp.broadcast_to(1.0 - jnp.max(gone, axis=1, keepdims=True), (BLOCKS, SLOTS))


def kernel(
    n_down,
    n_cross,
    count_ref,
    brick_ref,
    leave_ref,
    dest_ref,
    pos_ref,
    vel_ref,
    aff_ref,
    def_ref,
    weight_ref,
    mask_ref,
    state_ref,
    arrive_ref,
    early,
    early_in,
    late,
    late_in,
    table,
    chain,
    grid,
    node_v,
    movable,
    mask_y,
    mask_x_in,
    mask_y_in,
    mask_c_in,
    face_x,
    face_y,
    corner,
    sums,
    mass_ref,
    stay_ref,
    staged,
    scalars,
    scalar_sem,
    early_send,
    early_recv,
    late_send,
    late_recv,
    halo_send,
    halo_recv,
    mask_send,
    mask_recv,
):
    i = lax.axis_index("down")
    j = lax.axis_index("cross")

    def device(a, b):
        return (lax.rem(i + (a + n_down), n_down), lax.rem(j + (b + n_cross), n_cross))

    def inside(a, b):
        valid = None
        if a:
            valid = (i + a >= 0) & (i + a < n_down)
        if b:
            other = (j + b >= 0) & (j + b < n_cross)
            valid = other if valid is None else valid & other
        return valid.astype(f32)

    barrier = pltpu.get_barrier_semaphore()
    for a, b in move_list:
        pl.semaphore_signal(barrier, inc=1, device_id=device(a, b), device_id_type=MESH)

    build_tables(count_ref, brick_ref, leave_ref, dest_ref, weight_ref, mass_ref, stay_ref, staged)
    to_scalars = pltpu.make_async_copy(staged, scalars, scalar_sem)
    to_scalars.start()
    for par in range(2):
        mask_y[par] = mask_ref[pl.ds(par, 16, stride=16), :]
    to_scalars.wait()
    following = lambda b: scalars[0, b]
    first_of = lambda cell: scalars[1, cell]
    column_of = lambda b: scalars[2, b]
    lift_of = lambda b: scalars[3, b]
    source_of = lambda slot: scalars[4, slot]
    present_of = lambda slot: scalars[5, slot]

    def pick(move, carry):
        for k in range(8):
            source = source_of(move * 8 + k)
            early[move, 0:3, k : k + 1, :] = pos_ref[:, pl.ds(source, 1), :]
            early[move, 3:12, k : k + 1, :] = def_ref[:, pl.ds(source, 1), :]
            here = present_of(move * 8 + k).astype(f32)
            early[move, 12, k : k + 1, :] = mass_ref[pl.ds(source, 1), :] * here
        return carry

    lax.fori_loop(0, 8, pick, 0)

    def remote(source, target, send, recv, a, b):
        return pltpu.make_async_remote_copy(
            src_ref=source,
            dst_ref=target,
            send_sem=send,
            recv_sem=recv,
            device_id=device(a, b),
            device_id_type=MESH,
        )

    early_copies = [
        remote(early.at[m], early_in.at[m], early_send.at[m], early_recv.at[m], a, b)
        for m, (a, b) in enumerate(move_list)
    ]
    late_copies = [
        remote(late.at[m], late_in.at[m], late_send.at[m], late_recv.at[m], a, b)
        for m, (a, b) in enumerate(move_list)
    ]
    mask_copies = [
        remote(mask_y, mask_y_in, mask_send.at[0], mask_recv.at[0], 0, -1),
        remote(mask_ref.at[pl.ds(0, 32)], mask_x_in, mask_send.at[1], mask_recv.at[1], -1, 0),
        remote(mask_y.at[:, pl.ds(0, 8)], mask_c_in, mask_send.at[2], mask_recv.at[2], -1, -1),
    ]

    pl.semaphore_wait(barrier, 8)
    for copy in mask_copies:
        copy.start()
    for m in early_order[:early_first]:
        early_copies[m].start()

    def terms(g, carry):
        rows = pl.ds(pl.multiple_of(g * 8, 8), 8)
        deform = [def_ref[c, rows, :] for c in range(9)]
        affine = [aff_ref[c, rows, :] for c in range(9)]
        velocity = [vel_ref[c, rows, :] for c in range(3)]
        moved, columns = particle_rows(deform, affine, velocity, mass_ref[rows, :])
        zero = jnp.zeros((8, 128), f32)
        lists = [moved] + [[zero] + columns[c] for c in range(3)]
        for group, values in enumerate(lists):
            for quantity, value in enumerate(values):
                for par in range(2):
                    row = g * 256 + (8 * group + 2 * quantity + par)
                    table[pl.ds(row, 8, stride=32), :] = value
        return carry

    lax.fori_loop(0, 8, terms, 0)

    chain[BLOCKS] = jnp.zeros((64, 128), f32)

    def brick_sums(b):
        lift = lift_of(b)
        x0 = pos_ref[0, pl.ds(b, 1), :]
        x1 = pos_ref[1, pl.ds(b, 1), :]
        x2 = pos_ref[2, pl.ds(b, 1), :]
        base = pl.multiple_of(b * 32, 32)
        moved = table[pl.ds(base, 8), :]
        col0 = table[pl.ds(base + 8, 8), :]
        col1 = table[pl.ds(base + 16, 8), :]
        col2 = table[pl.ds(base + 24, 8), :]
        dx, wx, dy, wy = plane_weights(x0, x1)
        plain, raised = [], []
        for x in range(4):
            at_x = moved + col0 * dx[x]
            for yp in range(2):
                weight = wx[x] * wy[yp]
                plain.append((at_x + col1 * dy[yp]) * weight)
                raised.append(col2 * weight)
        lhs = jnp.concatenate([jnp.concatenate(plain, axis=0), jnp.concatenate(raised, axis=0)], axis=1)
        lhs_high, lhs_low = split(lhs)
        height = row_iota(8)
        dz = height.astype(f32) - x2
        wz = jnp.where(height + lift < GZ, spline(dz), 0.0)
        rhs = jnp.concatenate([wz, wz * dz], axis=1)
        rhs_high = rhs.astype(bf16).astype(f32)
        stacked = jnp.concatenate([rhs_high, rhs - rhs_high], axis=0).astype(bf16)
        contract = (((1,), (1,)), ((), ()))
        found = lax.dot_general(lhs_high, stacked, contract, preferred_element_type=f32)
        found = found + lax.dot_general(lhs_low, stacked, contract, preferred_element_type=f32)
        return lift, found

    def placed(lift, found):
        wide = jnp.concatenate([found, jnp.zeros((64, 112), f32)], axis=1)
        folded = pltpu.roll(wide, lift, 1) + pltpu.roll(wide, (lift + 120) & 127, 1)
        lane = lane_iota(64)
        return jnp.where((lane >= lift) & (lane < lift + 8), folded, 0.0)

    def to_bricks(step, carry):
        blocks = [(BLOCKS - 1) - (step * p2g_batch + u) for u in range(p2g_batch)]
        sums_of = [brick_sums(b) for b in blocks]
        out = [placed(*found) for found in sums_of]
        for b, value in zip(blocks, out):
            chain[b] = value + chain[following(b)]
        return carry

    lax.fori_loop(0, BLOCKS // p2g_batch, to_bricks, 0)

    def spread(p, carry):
        for q in range(9):
            cells = [[first_of((p + 1 - dp) * 10 + (q + 1 - dq)) for dq in range(2)] for dp in range(2)]
            for x in range(2):
                total = None
                for dp in range(2):
                    for dq in range(2):
                        start = 8 * (2 * (x + 2 * dp) + dq)
                        value = chain[cells[dp][dq], start : start + 8, :]
                        total = value if total is None else total + value
                grid[2 * p + x, q] = total
        return carry

    lax.fori_loop(0, 9, spread, 0)

    halo_copies = []
    faces = {-1: 0, 1: 1}
    for m, (a, b) in enumerate(move_list):
        xs = pl.ds(16, 2) if a == 1 else pl.ds(0, 2)
        y = 8 if b == 1 else 0
        if b == 0:
            source, target = grid.at[xs], face_x.at[faces[a]]
        elif a == 0:
            source, target = grid.at[:, y], face_y.at[faces[b]]
        else:
            source, target = grid.at[xs, y], corner.at[2 * faces[a] + faces[b]]
        halo_copies.append(remote(source, target, halo_send.at[m], halo_recv.at[m], a, b))
    for m in (3, 4, 0, 2, 5, 7, 1, 6):
        halo_copies[m].start()
    for m in early_order[early_first:]:
        early_copies[m].start()

    def own_mask(x, carry):
        movable[x, 0:16, :] = (1 - mask_ref[pl.ds(pl.multiple_of(x * 16, 16), 16), :]).astype(f32)
        return carry

    lax.fori_loop(0, 16, own_mask, 0)
    row8 = row_iota(8)
    even = (row8 & 1) == 0
    quantity = row8 // 2
    pull = jnp.where(quantity == 1, time_step * gravity[0], 0.0)
    pull = jnp.where(quantity == 2, time_step * gravity[1], pull)
    pull = jnp.where(quantity == 3, time_step * gravity[2], pull)

    def put_velocity(x, yp, tile):
        mass = jnp.where(row8 < 2, tile, 0.0)
        mass = mass + pltpu.roll(mass, 2, 0)
        mass = mass + pltpu.roll(mass, 4, 0)
        free = jnp.where(even, movable[x, pl.ds(2 * yp, 1), :], movable[x, pl.ds(2 * yp + 1, 1), :])
        node_v[x, yp] = free * (tile / jnp.maximum(mass, mass_floor) + pull)

    def interior(x, carry):
        for yp in range(1, 8):
            put_velocity(x, yp, grid[x, yp])
        return carry

    lax.fori_loop(2, 16, interior, 0)
    for copy in mask_copies:
        copy.wait()
    past_x = inside(1, 0)
    past_y = inside(0, 1)
    past_c = inside(1, 1)
    for xx in range(2):
        movable[16 + xx, 0:16, :] = (1 - mask_x_in[pl.ds(16 * xx, 16), :]).astype(f32) * past_x
        for par in range(2):
            movable[16 + xx, 16 + par : 17 + par, :] = (
                1 - mask_c_in[par, xx : xx + 1, :]
            ).astype(f32) * past_c

    def side_mask(x, carry):
        for par in range(2):
            movable[x, 16 + par : 17 + par, :] = (1 - mask_y_in[par, pl.ds(x, 1), :]).astype(f32) * past_y
        return carry

    lax.fori_loop(0, 16, side_mask, 0)
    for copy in halo_copies:
        copy.wait()
    has = {(a, b): inside(-a, -b) for a, b in move_list}

    def low_high(yp):
        for a in (-1, 1):
            for xx in range(2):
                x = xx if a == 1 else 16 + xx
                yield a, xx, x, grid[x, yp] + face_x[faces[a], xx, yp] * has[(a, 0)]

    def edge_x(yp, carry):
        for _, _, x, tile in low_high(yp):
            put_velocity(x, yp, tile)
        return carry

    lax.fori_loop(1, 8, edge_x, 0)

    def edge_y(x, carry):
        for b in (-1, 1):
            yp = 0 if b == 1 else 8
            put_velocity(x, yp, grid[x, yp] + face_y[faces[b], x] * has[(0, b)])
        return carry

    lax.fori_loop(2, 16, edge_y, 0)
    for b in (-1, 1):
        yp = 0 if b == 1 else 8
        for a, xx, x, tile in low_high(yp):
            tile = tile + face_y[faces[b], x] * has[(0, b)]
            tile = tile + corner[2 * faces[a] + faces[b], xx] * has[(a, b)]
            put_velocity(x, yp, tile)

    lane8 = lane_iota(8)

    def brick_tiles(b):
        column = column_of(b)
        p = column // NBY
        q = lax.rem(column, NBY)
        return [node_v[2 * p + x, q + yp] for x in range(4) for yp in range(2)]

    for move in range(8):

        packed = [jnp.zeros((8, 128), f32)] * 4
        for k in range(8):
            b = source_of(move * 8 + k)
            lift = lift_of(b)
            tiles = brick_tiles(b)
            shift = (8 * k + 128 - lift) & 127
            local = lane8 - 8 * k
            low = (local >= 0) & (local < 8) & (local + lift < GZ)
            local = local - 64
            high = (local >= 0) & (local < 8) & (local + lift < GZ)
            for t in range(4):
                kept = jnp.where(low, pltpu.roll(tiles[t], shift, 1), packed[t])
                packed[t] = jnp.where(high, pltpu.roll(tiles[t + 4], (shift + 64) & 127, 1), kept)
        for t in range(3):
            moved = pltpu.roll(packed[3], (8 - (2 + 2 * t)) & 7, 0)
            late[move, t] = jnp.where(row8 < 2, moved, packed[t])
        late_copies[move].start()

    lane64 = lane_iota(64)

    def windows(stack, shift):
        first = pltpu.roll(stack, shift & 127, 1)
        second = pltpu.roll(stack, (shift + 8) & 127, 1)
        third = pltpu.roll(stack, (shift + 16) & 127, 1)
        return jnp.where(lane64 < 8, first, jnp.where(lane64 < 16, second, third))

    def put_sums(b, total):
        base = pl.multiple_of(b * 32, 32)
        for t in range(4):
            sums[pl.ds(base + 8 * t, 8), :] = total[t]

    def resident(step, carry):
        blocks = [step * g2p_batch + u for u in range(g2p_batch)]
        totals = []
        for b in blocks:
            lift = lift_of(b)
            stack = jnp.concatenate(brick_tiles(b), axis=0)
            totals.append(
                gathered(
                    windows(stack, 128 - lift),
                    pos_ref[0, pl.ds(b, 1), :],
                    pos_ref[1, pl.ds(b, 1), :],
                    pos_ref[2, pl.ds(b, 1), :],
                    GZ - lift,
                )
            )
        for b, total in zip(blocks, totals):
            put_sums(b, total)
        return carry

    lax.fori_loop(0, BLOCKS // g2p_batch, resident, 0)

    def finish(g, carry):
        rows = pl.ds(pl.multiple_of(g * 8, 8), 8)
        position = [pos_ref[c, rows, :] for c in range(3)]
        deform = [def_ref[c, rows, :] for c in range(9)]
        keep = jnp.where(mass_ref[rows, :] > 0.0, stay_ref[rows, :], 0.0)
        for row, value in enumerate(final_rows(sums, g * 256, position, deform)):
            state_ref[row, rows, :] = value * keep
        return carry

    lax.fori_loop(0, 8, finish, 0)

    for move, (a, b) in enumerate(move_list):
        early_copies[move].wait()
        late_copies[move].wait()
        packed = [late_in[move, t] for t in range(3)]
        last = jnp.zeros((8, 128), f32)
        for t in range(3):
            last = last + pltpu.roll(jnp.where(row8 < 2, packed[t], 0.0), 2 + 2 * t, 0)
        packed.append(last)
        low_stack = jnp.concatenate(packed, axis=0)
        stack = jnp.concatenate([low_stack, pltpu.roll(low_stack, 64, 1)], axis=0)

        def arriving(step, carry, move=move, stack=stack):
            ks = [step * g2p_batch + u for u in range(g2p_batch)]
            totals = [
                gathered(
                    windows(stack, 128 - 8 * k),
                    early_in[move, 0, pl.ds(k, 1), :],
                    early_in[move, 1, pl.ds(k, 1), :],
                    early_in[move, 2, pl.ds(k, 1), :],
                    None,
                )
                for k in ks
            ]
            for k, total in zip(ks, totals):
                put_sums(k, total)
            return carry

        lax.fori_loop(0, 8 // g2p_batch, arriving, 0)
        rows = pl.ds(move * 8, 8)
        position = [early_in[move, c] for c in range(3)]
        deform = [early_in[move, 3 + c] for c in range(9)]
        mass = early_in[move, 12] * inside(-a, -b)
        keep = jnp.where(mass > 0.0, 1.0, 0.0)
        for row, value in enumerate(final_rows(sums, 0, position, deform)):
            arrive_ref[row, rows, :] = value * keep
        arrive_ref[24, rows, :] = mass


def body(
    n_down,
    n_cross,
    position,
    velocity,
    affine,
    deform,
    particle_mass,
    block_count,
    block_brick,
    boundary_mask,
    leaving_block,
    leaving_dest,
):
    vmem = pl.BlockSpec(memory_space=pltpu.VMEM)
    dma = pltpu.SemaphoreType.DMA
    return pl.pallas_call(
        functools.partial(kernel, n_down, n_cross),
        out_shape=(
            jax.ShapeDtypeStruct((24, BLOCKS, SLOTS), f32),
            jax.ShapeDtypeStruct((25, BLOCKS, SLOTS), f32),
        ),
        in_specs=[vmem] * 10,
        out_specs=(vmem, vmem),
        scratch_shapes=[
            pltpu.VMEM((8, 13, 8, 128), f32),
            pltpu.VMEM((8, 13, 8, 128), f32),
            pltpu.VMEM((8, 3, 8, 128), f32),
            pltpu.VMEM((8, 3, 8, 128), f32),
            pltpu.VMEM((BLOCKS * 32, 128), f32),
            pltpu.VMEM((BLOCKS + 1, 64, 128), f32),
            pltpu.VMEM((18, 9, 8, 128), f32),
            pltpu.VMEM((18, 9, 8, 128), f32),
            pltpu.VMEM((18, 24, 128), f32),
            pltpu.VMEM((2, 16, 128), jnp.int32),
            pltpu.VMEM((32, 128), jnp.int32),
            pltpu.VMEM((2, 16, 128), jnp.int32),
            pltpu.VMEM((2, 8, 128), jnp.int32),
            pltpu.VMEM((2, 2, 9, 8, 128), f32),
            pltpu.VMEM((2, 18, 8, 128), f32),
            pltpu.VMEM((4, 2, 8, 128), f32),
            pltpu.VMEM((BLOCKS * 32, 128), f32),
            pltpu.VMEM((BLOCKS, SLOTS), f32),
            pltpu.VMEM((BLOCKS, SLOTS), f32),
            pltpu.VMEM((8, 128), jnp.int32),
            pltpu.SMEM((8, 128), jnp.int32),
            dma,
            dma((8,)),
            dma((8,)),
            dma((8,)),
            dma((8,)),
            dma((8,)),
            dma((8,)),
            dma((3,)),
            dma((3,)),
        ],
        compiler_params=pltpu.CompilerParams(collective_id=0, has_side_effects=True),
    )(
        block_count.reshape(1, BLOCKS),
        block_brick.reshape(1, BLOCKS),
        leaving_block.reshape(1, BLOCKS),
        leaving_dest.reshape(1, BLOCKS),
        position,
        velocity,
        affine,
        deform,
        particle_mass,
        boundary_mask.reshape(GX * GY, GZ),
    )


def solution(mesh):
    blocks = P(None, ("down", "cross"), None)
    flat = P(("down", "cross"))
    in_specs = (
        blocks,
        blocks,
        blocks,
        blocks,
        P(("down", "cross"), None),
        flat,
        flat,
        P("down", "cross", None),
        flat,
        flat,
    )
    step = functools.partial(body, mesh.shape["down"], mesh.shape["cross"])
    return jax.shard_map(step, mesh=mesh, in_specs=in_specs, out_specs=(blocks, blocks), check_vma=False)
```

```python
import functools

import jax
import jax.numpy as jnp
from jax import lax
from jax.experimental import pallas as pl
from jax.experimental.pallas import tpu as pltpu
from jax.sharding import PartitionSpec as P

GX = 16
GY = 16
GZ = 128
SLOTS = 128
BLOCKS = 64
MIG = 8
NBX = 8
NBY = 8

time_step = 0.05
shear_modulus = 8.0
lame_first = 12.0
stress_factor = 0.2
gravity = (2.0, 0.0, -9.0)
mass_floor = 1.0
move_list = ((-1, -1), (-1, 0), (-1, 1), (0, -1), (0, 1), (1, -1), (1, 0), (1, 1))
early_order = (0, 2, 5, 7, 3, 4, 1, 6)
arrival_order = (1, 6, 0, 2, 5, 7, 3, 4)
early_first = 4
p2g_batch = 8
g2p_batch = 8

MESH = pl.DeviceIdType.MESH
f32 = jnp.float32
bf16 = jnp.bfloat16


def spline(distance):
    magnitude = jnp.abs(distance)
    outer_part = jnp.maximum(1.5 - magnitude, 0.0)
    return jnp.where(magnitude < 0.5, 0.75 - magnitude * magnitude, 0.5 * outer_part * outer_part)


def row_iota(rows):
    return lax.broadcasted_iota(jnp.int32, (rows, 128), 0)


def lane_iota(rows):
    return lax.broadcasted_iota(jnp.int32, (rows, 128), 1)


def plane_weights(x0, x1):
    parity = (row_iota(8) & 1).astype(f32)
    dx = [float(x) - x0 for x in range(4)]
    wx = [spline(d) for d in dx]
    dy = [(parity + 2.0 * yp) - x1 for yp in range(2)]
    wy = [spline(d) for d in dy]
    return dx, wx, dy, wy


def split(value):
    high = value.astype(bf16)
    low = (value - high.astype(f32)).astype(bf16)
    return high, low


def particle_rows(deform, affine, velocity, mass):
    d = deform
    determinant = (
        d[0] * (d[4] * d[8] - d[5] * d[7])
        - d[1] * (d[3] * d[8] - d[5] * d[6])
        + d[2] * (d[3] * d[7] - d[4] * d[6])
    )
    pressure = lame_first * jnp.log(determinant)
    columns = [[None] * 3 for _ in range(3)]
    for a in range(3):
        for c in range(a, 3):
            product = d[3 * a] * d[3 * c] + d[3 * a + 1] * d[3 * c + 1] + d[3 * a + 2] * d[3 * c + 2]
            if a == c:
                tau = shear_modulus * (product - 1.0) + pressure
            else:
                tau = shear_modulus * product
            columns[c][a] = mass * (affine[3 * a + c] - stress_factor * tau)
            if a != c:
                columns[a][c] = mass * (affine[3 * c + a] - stress_factor * tau)
    return [mass] + [mass * v for v in velocity], columns


def gathered(lhs_f32, x0, x1, x2, limit):
    lane = lane_iota(64)
    high = lhs_f32.astype(bf16).astype(f32)
    low = lhs_f32 - high
    lhs = jnp.where((lane >= 8) & (lane < 16), low, high)
    lhs = jnp.where(lane < 24, lhs, 0.0).astype(bf16)
    height = row_iota(8)
    dz = height.astype(f32) - x2
    wz = spline(dz)
    if limit is not None:
        wz = jnp.where(height < limit, wz, 0.0)
    rhs = jnp.concatenate([wz, wz * dz], axis=1)
    rhs_high = rhs.astype(bf16).astype(f32)
    rhs_low = rhs - rhs_high
    stacked = jnp.concatenate([rhs_high, rhs_high, rhs_low, jnp.zeros_like(rhs)], axis=0).astype(bf16)
    u = jnp.dot(lhs[:, :32], stacked, preferred_element_type=f32)
    dx, wx, dy, wy = plane_weights(x0, x1)
    wyd = [w * d for w, d in zip(wy, dy)]
    total = None
    for x in range(4):
        a = b = c = None
        for yp in range(2):
            start = 8 * (2 * x + yp)
            u0 = u[start : start + 8, :128]
            u1 = u[start : start + 8, 128:]
            terms = (wy[yp] * u0, wyd[yp] * u0, wy[yp] * u1)
            a, b, c = terms if a is None else (a + terms[0], b + terms[1], c + terms[2])
        parts = (wx[x] * a, (wx[x] * dx[x]) * a, wx[x] * b, wx[x] * c)
        total = parts if total is None else tuple(t + p for t, p in zip(total, parts))
    return total


def final_rows(sums_ref, base, position, deform):
    def both(row):
        return sums_ref[pl.ds(base + row, 8, stride=32), :] + sums_ref[pl.ds(base + row + 1, 8, stride=32), :]

    v = [both(2 + 2 * a) for a in range(3)]
    c = [4.0 * both(8 * (1 + col) + 2 + 2 * a) for a in range(3) for col in range(3)]
    x = [position[a] + time_step * v[a] for a in range(3)]
    f = []
    for a in range(3):
        for col in range(3):
            grown = c[3 * a] * deform[col] + c[3 * a + 1] * deform[3 + col] + c[3 * a + 2] * deform[6 + col]
            f.append(deform[3 * a + col] + time_step * grown)
    return x + v + c + f


def build_tables(count_ref, brick_ref, leave_ref, dest_ref, weight_ref, mass_ref, stay_ref, staged):
    shape = (128, 128)
    down = lax.broadcasted_iota(jnp.int32, shape, 0)
    across = lax.broadcasted_iota(jnp.int32, shape, 1)

    def padded(row, filler):
        return jnp.concatenate([row, jnp.full((1, 128 - BLOCKS), filler, jnp.int32)], axis=1)

    def upright(row):
        return jnp.transpose(jnp.broadcast_to(row, shape))

    def least(value):
        return jnp.min(value, axis=0, keepdims=True)

    count = upright(padded(count_ref[...], 0))[:BLOCKS]
    lane = across[:BLOCKS]
    mass_ref[...] = jnp.where(lane < count, weight_ref[...], 0.0)
    brick = padded(brick_ref[...], 0)
    column = brick >> 5
    sides = upright(column)[:BLOCKS]
    ids = down[:BLOCKS]
    staged[0:1, :] = least(jnp.where((sides == column) & (ids > lane), ids, BLOCKS))
    cell = ((sides >> 3) + 1) * 10 + (sides & 7) + 1
    staged[1:2, :] = least(jnp.where(cell == lane, ids, BLOCKS))
    staged[2:3, :] = column
    staged[3:4, :] = (brick & 31) * 4
    leave = padded(leave_ref[...], 0)
    dest = padded(dest_ref[...], 4)
    dest_up = upright(dest)[:BLOCKS]
    leave_up = upright(leave)[:BLOCKS]
    rank = jnp.sum(jnp.where((dest_up == dest) & (ids < lane), 1, 0), axis=0, keepdims=True)
    move = jnp.where(dest > 4, dest - 1, dest)
    slot = jnp.where(dest == 4, -1, move * 8 + rank)
    slot_up = upright(slot)[:BLOCKS]
    match = slot_up == lane
    staged[4:5, :] = jnp.sum(jnp.where(match, leave_up, 0), axis=0, keepdims=True)
    staged[5:6, :] = jnp.sum(jnp.where(match, 1, 0), axis=0, keepdims=True)
    staged[6:8, :] = jnp.zeros((2, 128), jnp.int32)
    gone = jnp.where((leave == ids) & (dest != 4), 1.0, 0.0)
    stay_ref[...] = jnp.broadcast_to(1.0 - jnp.max(gone, axis=1, keepdims=True), (BLOCKS, SLOTS))


def kernel(
    n_down,
    n_cross,
    count_ref,
    brick_ref,
    leave_ref,
    dest_ref,
    pos_hbm,
    vel_hbm,
    aff_hbm,
    def_hbm,
    weight_hbm,
    mask_hbm,
    state_out,
    arrive_out,
    pos_ref,
    vel_ref,
    aff_ref,
    def_ref,
    weight_ref,
    mask_ref,
    load_sem,
    state_ref,
    arrive_ref,
    out_sem,
    early,
    early_in,
    late,
    late_in,
    table,
    chain,
    grid,
    node_v,
    movable,
    mask_y,
    mask_x_in,
    mask_y_in,
    mask_c_in,
    face_x,
    face_y,
    corner,
    sums,
    mass_ref,
    stay_ref,
    staged,
    scalars,
    scalar_sem,
    early_send,
    early_recv,
    late_send,
    late_recv,
    halo_send,
    halo_recv,
    mask_send,
    mask_recv,
):
    loads = [
        pltpu.make_async_copy(source, target, load_sem.at[n])
        for n, (source, target) in enumerate(
            (
                (weight_hbm, weight_ref),
                (mask_hbm, mask_ref),
                (pos_hbm, pos_ref),
                (def_hbm, def_ref),
                (vel_hbm, vel_ref),
                (aff_hbm, aff_ref),
            )
        )
    ]
    for load in loads:
        load.start()
    i = lax.axis_index("down")
    j = lax.axis_index("cross")

    def device(a, b):
        return (lax.rem(i + (a + n_down), n_down), lax.rem(j + (b + n_cross), n_cross))

    def inside(a, b):
        valid = None
        if a:
            valid = (i + a >= 0) & (i + a < n_down)
        if b:
            other = (j + b >= 0) & (j + b < n_cross)
            valid = other if valid is None else valid & other
        return valid

    class Edge:
        def __init__(self, copy, a, b):
            self.copy, self.a, self.b = copy, a, b

        def start(self):
            pl.when(inside(self.a, self.b))(self.copy.start)

        def wait_send(self):
            pl.when(inside(self.a, self.b))(self.copy.wait_send)

        def wait_recv(self):
            pl.when(inside(-self.a, -self.b))(self.copy.wait_recv)

    barrier = pltpu.get_barrier_semaphore()
    neighbours = 0
    for a, b in move_list:

        @pl.when(inside(a, b))
        def greet(a=a, b=b):
            pl.semaphore_signal(barrier, inc=1, device_id=device(a, b), device_id_type=MESH)

        neighbours = neighbours + inside(a, b).astype(jnp.int32)

    def fill(target, a, b):
        @pl.when(jnp.logical_not(inside(a, b)))
        def zeros():
            target[...] = jnp.zeros(target.shape, target.dtype)

    for sign in (-1, 1):
        fill(face_x.at[(sign + 1) // 2], -sign, 0)
        fill(face_y.at[(sign + 1) // 2], 0, -sign)
        for other in (-1, 1):
            fill(corner.at[sign + 1 + (other + 1) // 2], -sign, -other)
    fill(mask_x_in, 1, 0)
    fill(mask_y_in, 0, 1)
    fill(mask_c_in, 1, 1)

    loads[0].wait()
    build_tables(count_ref, brick_ref, leave_ref, dest_ref, weight_ref, mass_ref, stay_ref, staged)
    to_scalars = pltpu.make_async_copy(staged, scalars, scalar_sem)
    to_scalars.start()
    loads[1].wait()
    for par in range(2):
        mask_y[par] = mask_ref[pl.ds(par, 16, stride=16), :]
    to_scalars.wait()
    loads[2].wait()
    loads[3].wait()
    following = lambda b: scalars[0, b]
    first_of = lambda cell: scalars[1, cell]
    column_of = lambda b: scalars[2, b]
    lift_of = lambda b: scalars[3, b]
    source_of = lambda slot: scalars[4, slot]
    present_of = lambda slot: scalars[5, slot]

    def pick(move, carry):
        for k in range(8):
            source = source_of(move * 8 + k)
            early[move, 0:3, k : k + 1, :] = pos_ref[:, pl.ds(source, 1), :]
            early[move, 3:12, k : k + 1, :] = def_ref[:, pl.ds(source, 1), :]
            here = present_of(move * 8 + k).astype(f32)
            early[move, 12, k : k + 1, :] = mass_ref[pl.ds(source, 1), :] * here
        return carry

    lax.fori_loop(0, 8, pick, 0)

    def remote(source, target, send, recv, a, b):
        copy = pltpu.make_async_remote_copy(
            src_ref=source,
            dst_ref=target,
            send_sem=send,
            recv_sem=recv,
            device_id=device(a, b),
            device_id_type=MESH,
        )
        return Edge(copy, a, b)

    early_copies = [
        remote(early.at[m], early_in.at[m], early_send.at[m], early_recv.at[m], a, b)
        for m, (a, b) in enumerate(move_list)
    ]
    late_copies = [
        remote(late.at[m], late_in.at[m], late_send.at[m], late_recv.at[m], a, b)
        for m, (a, b) in enumerate(move_list)
    ]
    mask_copies = [
        remote(mask_y, mask_y_in, mask_send.at[0], mask_recv.at[0], 0, -1),
        remote(mask_ref.at[pl.ds(0, 32)], mask_x_in, mask_send.at[1], mask_recv.at[1], -1, 0),
        remote(mask_y.at[:, pl.ds(0, 8)], mask_c_in, mask_send.at[2], mask_recv.at[2], -1, -1),
    ]

    def terms(g, carry):
        rows = pl.ds(pl.multiple_of(g * 8, 8), 8)
        deform = [def_ref[c, rows, :] for c in range(9)]
        affine = [aff_ref[c, rows, :] for c in range(9)]
        velocity = [vel_ref[c, rows, :] for c in range(3)]
        moved, columns = particle_rows(deform, affine, velocity, mass_ref[rows, :])
        zero = jnp.zeros((8, 128), f32)
        lists = [moved] + [[zero] + columns[c] for c in range(3)]
        for group, values in enumerate(lists):
            for quantity, value in enumerate(values):
                for par in range(2):
                    row = g * 256 + (8 * group + 2 * quantity + par)
                    table[pl.ds(row, 8, stride=32), :] = value
        return carry

    loads[4].wait()
    loads[5].wait()
    lax.fori_loop(0, 8, terms, 0)

    pl.semaphore_wait(barrier, neighbours)
    for copy in mask_copies:
        copy.start()
    for m in early_order[:early_first]:
        early_copies[m].start()

    chain[BLOCKS] = jnp.zeros((64, 128), f32)

    def brick_sums(b):
        lift = lift_of(b)
        x0 = pos_ref[0, pl.ds(b, 1), :]
        x1 = pos_ref[1, pl.ds(b, 1), :]
        x2 = pos_ref[2, pl.ds(b, 1), :]
        base = pl.multiple_of(b * 32, 32)
        moved = table[pl.ds(base, 8), :]
        col0 = table[pl.ds(base + 8, 8), :]
        col1 = table[pl.ds(base + 16, 8), :]
        col2 = table[pl.ds(base + 24, 8), :]
        dx, wx, dy, wy = plane_weights(x0, x1)
        plain, raised = [], []
        for x in range(4):
            at_x = moved + col0 * dx[x]
            for yp in range(2):
                weight = wx[x] * wy[yp]
                plain.append((at_x + col1 * dy[yp]) * weight)
                raised.append(col2 * weight)
        lhs = jnp.concatenate([jnp.concatenate(plain, axis=0), jnp.concatenate(raised, axis=0)], axis=1)
        lhs_high, lhs_low = split(lhs)
        height = row_iota(8)
        dz = height.astype(f32) - x2
        wz = jnp.where(height + lift < GZ, spline(dz), 0.0)
        rhs = jnp.concatenate([wz, wz * dz], axis=1)
        rhs_high = rhs.astype(bf16).astype(f32)
        stacked = jnp.concatenate([rhs_high, rhs - rhs_high], axis=0).astype(bf16)
        contract = (((1,), (1,)), ((), ()))
        found = lax.dot_general(lhs_high, stacked, contract, preferred_element_type=f32)
        found = found + lax.dot_general(lhs_low, stacked, contract, preferred_element_type=f32)
        return lift, found

    def placed(lift, found):
        wide = jnp.concatenate([found, jnp.zeros((64, 112), f32)], axis=1)
        folded = pltpu.roll(wide, lift, 1) + pltpu.roll(wide, (lift + 120) & 127, 1)
        lane = lane_iota(64)
        return jnp.where((lane >= lift) & (lane < lift + 8), folded, 0.0)

    def to_bricks(step, carry):
        blocks = [(BLOCKS - 1) - (step * p2g_batch + u) for u in range(p2g_batch)]
        sums_of = [brick_sums(b) for b in blocks]
        out = [placed(*found) for found in sums_of]
        for b, value in zip(blocks, out):
            chain[b] = value + chain[following(b)]
        return carry

    lax.fori_loop(0, BLOCKS // p2g_batch, to_bricks, 0)

    def spread(p, carry):
        for q in range(9):
            cells = [[first_of((p + 1 - dp) * 10 + (q + 1 - dq)) for dq in range(2)] for dp in range(2)]
            for x in range(2):
                total = None
                for dp in range(2):
                    for dq in range(2):
                        start = 8 * (2 * (x + 2 * dp) + dq)
                        value = chain[cells[dp][dq], start : start + 8, :]
                        total = value if total is None else total + value
                grid[2 * p + x, q] = total
        return carry

    lax.fori_loop(0, 9, spread, 0)

    halo_copies = []
    faces = {-1: 0, 1: 1}
    for m, (a, b) in enumerate(move_list):
        xs = pl.ds(16, 2) if a == 1 else pl.ds(0, 2)
        y = 8 if b == 1 else 0
        if b == 0:
            source, target = grid.at[xs], face_x.at[faces[a]]
        elif a == 0:
            source, target = grid.at[:, y], face_y.at[faces[b]]
        else:
            source, target = grid.at[xs, y], corner.at[2 * faces[a] + faces[b]]
        halo_copies.append(remote(source, target, halo_send.at[m], halo_recv.at[m], a, b))
    for m in (3, 4, 0, 2, 5, 7, 1, 6):
        halo_copies[m].start()
    for m in early_order[early_first:]:
        early_copies[m].start()

    def own_mask(x, carry):
        movable[x, 0:16, :] = (1 - mask_ref[pl.ds(pl.multiple_of(x * 16, 16), 16), :]).astype(f32)
        return carry

    lax.fori_loop(0, 16, own_mask, 0)
    row8 = row_iota(8)
    even = (row8 & 1) == 0
    quantity = row8 // 2
    pull = jnp.where(quantity == 1, time_step * gravity[0], 0.0)
    pull = jnp.where(quantity == 2, time_step * gravity[1], pull)
    pull = jnp.where(quantity == 3, time_step * gravity[2], pull)

    def put_velocity(x, yp, tile):
        mass = jnp.where(row8 < 2, tile, 0.0)
        mass = mass + pltpu.roll(mass, 2, 0)
        mass = mass + pltpu.roll(mass, 4, 0)
        free = jnp.where(even, movable[x, pl.ds(2 * yp, 1), :], movable[x, pl.ds(2 * yp + 1, 1), :])
        node_v[x, yp] = free * (tile / jnp.maximum(mass, mass_floor) + pull)

    def interior(x, carry):
        for yp in range(1, 8):
            put_velocity(x, yp, grid[x, yp])
        return carry

    lax.fori_loop(2, 16, interior, 0)
    for copy in mask_copies:
        copy.wait_recv()
    past_x = inside(1, 0).astype(f32)
    past_y = inside(0, 1).astype(f32)
    past_c = inside(1, 1).astype(f32)
    for xx in range(2):
        movable[16 + xx, 0:16, :] = (1 - mask_x_in[pl.ds(16 * xx, 16), :]).astype(f32) * past_x
        for par in range(2):
            movable[16 + xx, 16 + par : 17 + par, :] = (
                1 - mask_c_in[par, xx : xx + 1, :]
            ).astype(f32) * past_c

    def side_mask(x, carry):
        for par in range(2):
            movable[x, 16 + par : 17 + par, :] = (1 - mask_y_in[par, pl.ds(x, 1), :]).astype(f32) * past_y
        return carry

    lax.fori_loop(0, 16, side_mask, 0)
    for copy in halo_copies:
        copy.wait_recv()

    def low_high(yp):
        for a in (-1, 1):
            for xx in range(2):
                x = xx if a == 1 else 16 + xx
                yield a, xx, x, grid[x, yp] + face_x[faces[a], xx, yp]

    def edge_x(yp, carry):
        for _, _, x, tile in low_high(yp):
            put_velocity(x, yp, tile)
        return carry

    lax.fori_loop(1, 8, edge_x, 0)

    def edge_y(x, carry):
        for b in (-1, 1):
            yp = 0 if b == 1 else 8
            put_velocity(x, yp, grid[x, yp] + face_y[faces[b], x])
        return carry

    lax.fori_loop(2, 16, edge_y, 0)
    for b in (-1, 1):
        yp = 0 if b == 1 else 8
        for a, xx, x, tile in low_high(yp):
            tile = tile + face_y[faces[b], x]
            tile = tile + corner[2 * faces[a] + faces[b], xx]
            put_velocity(x, yp, tile)

    lane8 = lane_iota(8)

    def brick_tiles(b):
        column = column_of(b)
        p = column // NBY
        q = lax.rem(column, NBY)
        return [node_v[2 * p + x, q + yp] for x in range(4) for yp in range(2)]

    for move in early_order:
        packed = [jnp.zeros((8, 128), f32)] * 4
        for k in range(8):
            b = source_of(move * 8 + k)
            lift = lift_of(b)
            tiles = brick_tiles(b)
            shift = (8 * k + 128 - lift) & 127
            local = lane8 - 8 * k
            low = (local >= 0) & (local < 8) & (local + lift < GZ)
            local = local - 64
            high = (local >= 0) & (local < 8) & (local + lift < GZ)
            for t in range(4):
                kept = jnp.where(low, pltpu.roll(tiles[t], shift, 1), packed[t])
                packed[t] = jnp.where(high, pltpu.roll(tiles[t + 4], (shift + 64) & 127, 1), kept)
        for t in range(3):
            moved = pltpu.roll(packed[3], (8 - (2 + 2 * t)) & 7, 0)
            late[move, t] = jnp.where(row8 < 2, moved, packed[t])
        late_copies[move].start()

    lane64 = lane_iota(64)

    def windows(stack, shift):
        first = pltpu.roll(stack, shift & 127, 1)
        second = pltpu.roll(stack, (shift + 8) & 127, 1)
        third = pltpu.roll(stack, (shift + 16) & 127, 1)
        return jnp.where(lane64 < 8, first, jnp.where(lane64 < 16, second, third))

    def put_sums(b, total):
        base = pl.multiple_of(b * 32, 32)
        for t in range(4):
            sums[pl.ds(base + 8 * t, 8), :] = total[t]

    def resident(step, carry):
        blocks = [step * g2p_batch + u for u in range(g2p_batch)]
        totals = []
        for b in blocks:
            lift = lift_of(b)
            stack = jnp.concatenate(brick_tiles(b), axis=0)
            totals.append(
                gathered(
                    windows(stack, 128 - lift),
                    pos_ref[0, pl.ds(b, 1), :],
                    pos_ref[1, pl.ds(b, 1), :],
                    pos_ref[2, pl.ds(b, 1), :],
                    GZ - lift,
                )
            )
        for b, total in zip(blocks, totals):
            put_sums(b, total)
        return carry

    lax.fori_loop(0, BLOCKS // g2p_batch, resident, 0)

    def finish(g, carry):
        rows = pl.ds(pl.multiple_of(g * 8, 8), 8)
        position = [pos_ref[c, rows, :] for c in range(3)]
        deform = [def_ref[c, rows, :] for c in range(9)]
        keep = jnp.where(mass_ref[rows, :] > 0.0, stay_ref[rows, :], 0.0)
        for row, value in enumerate(final_rows(sums, g * 256, position, deform)):
            state_ref[row, rows, :] = value * keep
        return carry

    lax.fori_loop(0, 8, finish, 0)
    stores = [pltpu.make_async_copy(state_ref, state_out, out_sem.at[8])]
    stores[0].start()

    for move in arrival_order:
        a, b = move_list[move]
        early_copies[move].wait_recv()
        late_copies[move].wait_recv()
        rows = pl.ds(move * 8, 8)

        @pl.when(jnp.logical_not(inside(-a, -b)))
        def nobody(rows=rows):
            arrive_ref[:, rows, :] = jnp.zeros((25, 8, 128), f32)

        @pl.when(inside(-a, -b))
        def somebody(move=move, rows=rows):
            packed = [late_in[move, t] for t in range(3)]
            last = jnp.zeros((8, 128), f32)
            for t in range(3):
                last = last + pltpu.roll(jnp.where(row8 < 2, packed[t], 0.0), 2 + 2 * t, 0)
            packed.append(last)
            low_stack = jnp.concatenate(packed, axis=0)
            stack = jnp.concatenate([low_stack, pltpu.roll(low_stack, 64, 1)], axis=0)

            def arriving(step, carry, move=move, stack=stack):
                ks = [step * g2p_batch + u for u in range(g2p_batch)]
                totals = [
                    gathered(
                        windows(stack, 128 - 8 * k),
                        early_in[move, 0, pl.ds(k, 1), :],
                        early_in[move, 1, pl.ds(k, 1), :],
                        early_in[move, 2, pl.ds(k, 1), :],
                        None,
                    )
                    for k in ks
                ]
                for k, total in zip(ks, totals):
                    put_sums(k, total)
                return carry

            lax.fori_loop(0, 8 // g2p_batch, arriving, 0)
            position = [early_in[move, c] for c in range(3)]
            deform = [early_in[move, 3 + c] for c in range(9)]
            mass = early_in[move, 12]
            keep = jnp.where(mass > 0.0, 1.0, 0.0)
            for row, value in enumerate(final_rows(sums, 0, position, deform)):
                arrive_ref[row, rows, :] = value * keep
            arrive_ref[24, rows, :] = mass

        store = pltpu.make_async_copy(arrive_ref.at[:, rows], arrive_out.at[:, rows], out_sem.at[move])
        store.start()
        stores.append(store)
    for copy in early_copies + late_copies + halo_copies + mask_copies:
        copy.wait_send()
    for store in stores:
        store.wait()


def pass_on(state, arrivals, state_out, arrive_out, held, held_too, in_sem, out_sem):
    chunks = [(state, held, state_out, pl.ds(6 * n, 6)) for n in range(4)]
    chunks += [(arrivals, held_too, arrive_out, pl.ds(5 * n, 5)) for n in range(5)]
    taken = [pltpu.make_async_copy(a.at[d], v.at[d], in_sem.at[n]) for n, (a, v, _, d) in enumerate(chunks)]
    given = [pltpu.make_async_copy(v.at[d], o.at[d], out_sem.at[n]) for n, (_, v, o, d) in enumerate(chunks)]
    for copy in taken:
        copy.start()
    for copy, onward in zip(taken, given):
        copy.wait()
        onward.start()
    for onward in given:
        onward.wait()


def body(
    n_down,
    n_cross,
    position,
    velocity,
    affine,
    deform,
    particle_mass,
    block_count,
    block_brick,
    boundary_mask,
    leaving_block,
    leaving_dest,
):
    vmem = pl.BlockSpec(memory_space=pltpu.VMEM)
    dma = pltpu.SemaphoreType.DMA
    hbm = pl.BlockSpec(memory_space=pltpu.HBM)
    results = pl.pallas_call(
        functools.partial(kernel, n_down, n_cross),
        out_shape=(
            jax.ShapeDtypeStruct((24, BLOCKS, SLOTS), f32),
            jax.ShapeDtypeStruct((25, BLOCKS, SLOTS), f32),
        ),
        in_specs=[vmem] * 4 + [pl.BlockSpec(memory_space=pltpu.HBM)] * 6,
        out_specs=(hbm, hbm),
        scratch_shapes=[
            pltpu.VMEM((3, BLOCKS, SLOTS), f32),
            pltpu.VMEM((3, BLOCKS, SLOTS), f32),
            pltpu.VMEM((9, BLOCKS, SLOTS), f32),
            pltpu.VMEM((9, BLOCKS, SLOTS), f32),
            pltpu.VMEM((BLOCKS, SLOTS), f32),
            pltpu.VMEM((GX * GY, GZ), jnp.int32),
            dma((6,)),
            pltpu.VMEM((24, BLOCKS, SLOTS), f32),
            pltpu.VMEM((25, BLOCKS, SLOTS), f32),
            dma((9,)),
            pltpu.VMEM((8, 13, 8, 128), f32),
            pltpu.VMEM((8, 13, 8, 128), f32),
            pltpu.VMEM((8, 3, 8, 128), f32),
            pltpu.VMEM((8, 3, 8, 128), f32),
            pltpu.VMEM((BLOCKS * 32, 128), f32),
            pltpu.VMEM((BLOCKS + 1, 64, 128), f32),
            pltpu.VMEM((18, 9, 8, 128), f32),
            pltpu.VMEM((18, 9, 8, 128), f32),
            pltpu.VMEM((18, 24, 128), f32),
            pltpu.VMEM((2, 16, 128), jnp.int32),
            pltpu.VMEM((32, 128), jnp.int32),
            pltpu.VMEM((2, 16, 128), jnp.int32),
            pltpu.VMEM((2, 8, 128), jnp.int32),
            pltpu.VMEM((2, 2, 9, 8, 128), f32),
            pltpu.VMEM((2, 18, 8, 128), f32),
            pltpu.VMEM((4, 2, 8, 128), f32),
            pltpu.VMEM((BLOCKS * 32, 128), f32),
            pltpu.VMEM((BLOCKS, SLOTS), f32),
            pltpu.VMEM((BLOCKS, SLOTS), f32),
            pltpu.VMEM((8, 128), jnp.int32),
            pltpu.SMEM((8, 128), jnp.int32),
            dma,
            dma((8,)),
            dma((8,)),
            dma((8,)),
            dma((8,)),
            dma((8,)),
            dma((8,)),
            dma((3,)),
            dma((3,)),
        ],
        compiler_params=pltpu.CompilerParams(collective_id=0, has_side_effects=True),
    )(
        block_count.reshape(1, BLOCKS),
        block_brick.reshape(1, BLOCKS),
        leaving_block.reshape(1, BLOCKS),
        leaving_dest.reshape(1, BLOCKS),
        position,
        velocity,
        affine,
        deform,
        particle_mass,
        boundary_mask.reshape(GX * GY, GZ),
    )
    return pl.pallas_call(
        pass_on,
        out_shape=(
            jax.ShapeDtypeStruct((24, BLOCKS, SLOTS), f32),
            jax.ShapeDtypeStruct((25, BLOCKS, SLOTS), f32),
        ),
        in_specs=[hbm, hbm],
        out_specs=(hbm, hbm),
        scratch_shapes=[
            pltpu.VMEM((24, BLOCKS, SLOTS), f32),
            pltpu.VMEM((25, BLOCKS, SLOTS), f32),
            dma((9,)),
            dma((9,)),
        ],
    )(*results)


def solution(mesh):
    blocks = P(None, ("down", "cross"), None)
    flat = P(("down", "cross"))
    in_specs = (
        blocks,
        blocks,
        blocks,
        blocks,
        P(("down", "cross"), None),
        flat,
        flat,
        P("down", "cross", None),
        flat,
        flat,
    )
    step = functools.partial(body, mesh.shape["down"], mesh.shape["cross"])
    return jax.shard_map(step, mesh=mesh, in_specs=in_specs, out_specs=(blocks, blocks), check_vma=False)
```

```python
import functools

import jax
import jax.numpy as jnp
from jax import lax
from jax.experimental import pallas as pl
from jax.experimental.pallas import tpu as pltpu
from jax.sharding import PartitionSpec as P

GX = 16
GY = 16
GZ = 128
SLOTS = 128
BLOCKS = 64
MIG = 8
NBX = 8
NBY = 8

time_step = 0.05
shear_modulus = 8.0
lame_first = 12.0
stress_factor = 0.2
gravity = (2.0, 0.0, -9.0)
mass_floor = 1.0
move_list = ((-1, -1), (-1, 0), (-1, 1), (0, -1), (0, 1), (1, -1), (1, 0), (1, 1))
early_order = (0, 2, 5, 7, 3, 4, 1, 6)
arrival_order = (1, 6, 0, 2, 5, 7, 3, 4)
early_first = 4
p2g_batch = 8
g2p_batch = 8

MESH = pl.DeviceIdType.MESH
f32 = jnp.float32
bf16 = jnp.bfloat16


def spline(distance):
    magnitude = jnp.abs(distance)
    outer_part = jnp.maximum(1.5 - magnitude, 0.0)
    return jnp.where(magnitude < 0.5, 0.75 - magnitude * magnitude, 0.5 * outer_part * outer_part)


def row_iota(rows):
    return lax.broadcasted_iota(jnp.int32, (rows, 128), 0)


def lane_iota(rows):
    return lax.broadcasted_iota(jnp.int32, (rows, 128), 1)


def plane_weights(x0, x1):
    parity = (row_iota(8) & 1).astype(f32)
    dx = [float(x) - x0 for x in range(4)]
    wx = [spline(d) for d in dx]
    dy = [(parity + 2.0 * yp) - x1 for yp in range(2)]
    wy = [spline(d) for d in dy]
    return dx, wx, dy, wy


def split(value):
    high = value.astype(bf16)
    low = (value - high.astype(f32)).astype(bf16)
    return high, low


def particle_rows(deform, affine, velocity, mass):
    d = deform
    determinant = (
        d[0] * (d[4] * d[8] - d[5] * d[7])
        - d[1] * (d[3] * d[8] - d[5] * d[6])
        + d[2] * (d[3] * d[7] - d[4] * d[6])
    )
    pressure = lame_first * jnp.log(determinant)
    columns = [[None] * 3 for _ in range(3)]
    for a in range(3):
        for c in range(a, 3):
            product = d[3 * a] * d[3 * c] + d[3 * a + 1] * d[3 * c + 1] + d[3 * a + 2] * d[3 * c + 2]
            if a == c:
                tau = shear_modulus * (product - 1.0) + pressure
            else:
                tau = shear_modulus * product
            columns[c][a] = mass * (affine[3 * a + c] - stress_factor * tau)
            if a != c:
                columns[a][c] = mass * (affine[3 * c + a] - stress_factor * tau)
    return [mass] + [mass * v for v in velocity], columns


def gathered(lhs_f32, x0, x1, x2, limit):
    lane = lane_iota(64)
    high = lhs_f32.astype(bf16).astype(f32)
    low = lhs_f32 - high
    lhs = jnp.where((lane >= 8) & (lane < 16), low, high)
    lhs = jnp.where(lane < 24, lhs, 0.0).astype(bf16)
    height = row_iota(8)
    dz = height.astype(f32) - x2
    wz = spline(dz)
    if limit is not None:
        wz = jnp.where(height < limit, wz, 0.0)
    rhs = jnp.concatenate([wz, wz * dz], axis=1)
    rhs_high = rhs.astype(bf16).astype(f32)
    rhs_low = rhs - rhs_high
    stacked = jnp.concatenate([rhs_high, rhs_high, rhs_low, jnp.zeros_like(rhs)], axis=0).astype(bf16)
    u = jnp.dot(lhs[:, :32], stacked, preferred_element_type=f32)
    dx, wx, dy, wy = plane_weights(x0, x1)
    wyd = [w * d for w, d in zip(wy, dy)]
    total = None
    for x in range(4):
        a = b = c = None
        for yp in range(2):
            start = 8 * (2 * x + yp)
            u0 = u[start : start + 8, :128]
            u1 = u[start : start + 8, 128:]
            terms = (wy[yp] * u0, wyd[yp] * u0, wy[yp] * u1)
            a, b, c = terms if a is None else (a + terms[0], b + terms[1], c + terms[2])
        parts = (wx[x] * a, (wx[x] * dx[x]) * a, wx[x] * b, wx[x] * c)
        total = parts if total is None else tuple(t + p for t, p in zip(total, parts))
    return total


def final_rows(sums_ref, base, position, deform):
    def both(row):
        return sums_ref[pl.ds(base + row, 8, stride=32), :] + sums_ref[pl.ds(base + row + 1, 8, stride=32), :]

    v = [both(2 + 2 * a) for a in range(3)]
    c = [4.0 * both(8 * (1 + col) + 2 + 2 * a) for a in range(3) for col in range(3)]
    x = [position[a] + time_step * v[a] for a in range(3)]
    f = []
    for a in range(3):
        for col in range(3):
            grown = c[3 * a] * deform[col] + c[3 * a + 1] * deform[3 + col] + c[3 * a + 2] * deform[6 + col]
            f.append(deform[3 * a + col] + time_step * grown)
    return x + v + c + f


def build_tables(count_ref, brick_ref, leave_ref, dest_ref, weight_ref, mass_ref, stay_ref, staged):
    shape = (128, 128)
    down = lax.broadcasted_iota(jnp.int32, shape, 0)
    across = lax.broadcasted_iota(jnp.int32, shape, 1)

    def padded(row, filler):
        return jnp.concatenate([row, jnp.full((1, 128 - BLOCKS), filler, jnp.int32)], axis=1)

    def upright(row):
        return jnp.transpose(jnp.broadcast_to(row, shape))

    def least(value):
        return jnp.min(value, axis=0, keepdims=True)

    count = upright(padded(count_ref[...], 0))[:BLOCKS]
    lane = across[:BLOCKS]
    mass_ref[...] = jnp.where(lane < count, weight_ref[...], 0.0)
    brick = padded(brick_ref[...], 0)
    column = brick >> 5
    sides = upright(column)[:BLOCKS]
    ids = down[:BLOCKS]
    staged[0:1, :] = least(jnp.where((sides == column) & (ids > lane), ids, BLOCKS))
    cell = ((sides >> 3) + 1) * 10 + (sides & 7) + 1
    staged[1:2, :] = least(jnp.where(cell == lane, ids, BLOCKS))
    staged[2:3, :] = column
    staged[3:4, :] = (brick & 31) * 4
    leave = padded(leave_ref[...], 0)
    dest = padded(dest_ref[...], 4)
    dest_up = upright(dest)[:BLOCKS]
    leave_up = upright(leave)[:BLOCKS]
    rank = jnp.sum(jnp.where((dest_up == dest) & (ids < lane), 1, 0), axis=0, keepdims=True)
    move = jnp.where(dest > 4, dest - 1, dest)
    slot = jnp.where(dest == 4, -1, move * 8 + rank)
    slot_up = upright(slot)[:BLOCKS]
    match = slot_up == lane
    staged[4:5, :] = jnp.sum(jnp.where(match, leave_up, 0), axis=0, keepdims=True)
    staged[5:6, :] = jnp.sum(jnp.where(match, 1, 0), axis=0, keepdims=True)
    staged[6:8, :] = jnp.zeros((2, 128), jnp.int32)
    gone = jnp.where((leave == ids) & (dest != 4), 1.0, 0.0)
    stay_ref[...] = jnp.broadcast_to(1.0 - jnp.max(gone, axis=1, keepdims=True), (BLOCKS, SLOTS))


def kernel(
    n_down,
    n_cross,
    count_ref,
    brick_ref,
    leave_ref,
    dest_ref,
    pos_hbm,
    vel_hbm,
    aff_hbm,
    def_hbm,
    weight_hbm,
    mask_hbm,
    state_out,
    arrive_out,
    pos_ref,
    vel_ref,
    aff_ref,
    def_ref,
    weight_ref,
    mask_ref,
    load_sem,
    state_ref,
    arrive_ref,
    out_sem,
    early,
    early_in,
    late,
    late_in,
    table,
    chain,
    grid,
    node_v,
    movable,
    mask_y,
    mask_x_in,
    mask_y_in,
    mask_c_in,
    face_x,
    face_y,
    corner,
    sums,
    mass_ref,
    stay_ref,
    staged,
    scalars,
    scalar_sem,
    early_send,
    early_recv,
    late_send,
    late_recv,
    halo_send,
    halo_recv,
    mask_send,
    mask_recv,
):
    loads = [
        pltpu.make_async_copy(source, target, load_sem.at[n])
        for n, (source, target) in enumerate(
            (
                (weight_hbm, weight_ref),
                (mask_hbm, mask_ref),
                (pos_hbm, pos_ref),
                (def_hbm, def_ref),
                (vel_hbm, vel_ref),
                (aff_hbm, aff_ref),
            )
        )
    ]
    for load in loads:
        load.start()
    i = lax.axis_index("down")
    j = lax.axis_index("cross")

    def device(a, b):
        return (lax.rem(i + (a + n_down), n_down), lax.rem(j + (b + n_cross), n_cross))

    def inside(a, b):
        valid = None
        if a:
            valid = (i + a >= 0) & (i + a < n_down)
        if b:
            other = (j + b >= 0) & (j + b < n_cross)
            valid = other if valid is None else valid & other
        return valid

    class Edge:
        def __init__(self, copy, a, b):
            self.copy, self.a, self.b = copy, a, b

        def start(self):
            pl.when(inside(self.a, self.b))(self.copy.start)

        def wait_send(self):
            pl.when(inside(self.a, self.b))(self.copy.wait_send)

        def wait_recv(self):
            pl.when(inside(-self.a, -self.b))(self.copy.wait_recv)

    barrier = pltpu.get_barrier_semaphore()
    neighbours = 0
    for a, b in move_list:

        @pl.when(inside(a, b))
        def greet(a=a, b=b):
            pl.semaphore_signal(barrier, inc=1, device_id=device(a, b), device_id_type=MESH)

        neighbours = neighbours + inside(a, b).astype(jnp.int32)

    def fill(target, a, b):
        @pl.when(jnp.logical_not(inside(a, b)))
        def zeros():
            target[...] = jnp.zeros(target.shape, target.dtype)

    for sign in (-1, 1):
        fill(face_x.at[(sign + 1) // 2], -sign, 0)
        fill(face_y.at[(sign + 1) // 2], 0, -sign)
        for other in (-1, 1):
            fill(corner.at[sign + 1 + (other + 1) // 2], -sign, -other)
    fill(mask_x_in, 1, 0)
    fill(mask_y_in, 0, 1)
    fill(mask_c_in, 1, 1)

    loads[0].wait()
    build_tables(count_ref, brick_ref, leave_ref, dest_ref, weight_ref, mass_ref, stay_ref, staged)
    to_scalars = pltpu.make_async_copy(staged, scalars, scalar_sem)
    to_scalars.start()
    loads[1].wait()
    for par in range(2):
        mask_y[par] = mask_ref[pl.ds(par, 16, stride=16), :]
    to_scalars.wait()
    loads[2].wait()
    loads[3].wait()
    following = lambda b: scalars[0, b]
    first_of = lambda cell: scalars[1, cell]
    column_of = lambda b: scalars[2, b]
    lift_of = lambda b: scalars[3, b]
    source_of = lambda slot: scalars[4, slot]
    present_of = lambda slot: scalars[5, slot]

    def pick(move, carry):
        for k in range(8):
            source = source_of(move * 8 + k)
            early[move, 0:3, k : k + 1, :] = pos_ref[:, pl.ds(source, 1), :]
            early[move, 3:12, k : k + 1, :] = def_ref[:, pl.ds(source, 1), :]
            here = present_of(move * 8 + k).astype(f32)
            early[move, 12, k : k + 1, :] = mass_ref[pl.ds(source, 1), :] * here
        return carry

    lax.fori_loop(0, 8, pick, 0)

    def remote(source, target, send, recv, a, b):
        copy = pltpu.make_async_remote_copy(
            src_ref=source,
            dst_ref=target,
            send_sem=send,
            recv_sem=recv,
            device_id=device(a, b),
            device_id_type=MESH,
        )
        return Edge(copy, a, b)

    early_copies = [
        remote(early.at[m], early_in.at[m], early_send.at[m], early_recv.at[m], a, b)
        for m, (a, b) in enumerate(move_list)
    ]
    late_copies = [
        remote(late.at[m], late_in.at[m], late_send.at[m], late_recv.at[m], a, b)
        for m, (a, b) in enumerate(move_list)
    ]
    mask_copies = [
        remote(mask_y, mask_y_in, mask_send.at[0], mask_recv.at[0], 0, -1),
        remote(mask_ref.at[pl.ds(0, 32)], mask_x_in, mask_send.at[1], mask_recv.at[1], -1, 0),
        remote(mask_y.at[:, pl.ds(0, 8)], mask_c_in, mask_send.at[2], mask_recv.at[2], -1, -1),
    ]

    pl.semaphore_wait(barrier, neighbours)
    for m in early_order[:early_first]:
        early_copies[m].start()

    def terms(g, carry):
        rows = pl.ds(pl.multiple_of(g * 8, 8), 8)
        deform = [def_ref[c, rows, :] for c in range(9)]
        affine = [aff_ref[c, rows, :] for c in range(9)]
        velocity = [vel_ref[c, rows, :] for c in range(3)]
        moved, columns = particle_rows(deform, affine, velocity, mass_ref[rows, :])
        zero = jnp.zeros((8, 128), f32)
        lists = [moved] + [[zero] + columns[c] for c in range(3)]
        for group, values in enumerate(lists):
            for quantity, value in enumerate(values):
                for par in range(2):
                    row = g * 256 + (8 * group + 2 * quantity + par)
                    table[pl.ds(row, 8, stride=32), :] = value
        return carry

    loads[4].wait()
    loads[5].wait()
    lax.fori_loop(0, 8, terms, 0)

    chain[BLOCKS] = jnp.zeros((64, 128), f32)

    def brick_sums(b):
        lift = lift_of(b)
        x0 = pos_ref[0, pl.ds(b, 1), :]
        x1 = pos_ref[1, pl.ds(b, 1), :]
        x2 = pos_ref[2, pl.ds(b, 1), :]
        base = pl.multiple_of(b * 32, 32)
        moved = table[pl.ds(base, 8), :]
        col0 = table[pl.ds(base + 8, 8), :]
        col1 = table[pl.ds(base + 16, 8), :]
        col2 = table[pl.ds(base + 24, 8), :]
        dx, wx, dy, wy = plane_weights(x0, x1)
        plain, raised = [], []
        for x in range(4):
            at_x = moved + col0 * dx[x]
            for yp in range(2):
                weight = wx[x] * wy[yp]
                plain.append((at_x + col1 * dy[yp]) * weight)
                raised.append(col2 * weight)
        lhs = jnp.concatenate([jnp.concatenate(plain, axis=0), jnp.concatenate(raised, axis=0)], axis=1)
        lhs_high, lhs_low = split(lhs)
        height = row_iota(8)
        dz = height.astype(f32) - x2
        wz = jnp.where(height + lift < GZ, spline(dz), 0.0)
        rhs = jnp.concatenate([wz, wz * dz], axis=1)
        rhs_high = rhs.astype(bf16).astype(f32)
        stacked = jnp.concatenate([rhs_high, rhs - rhs_high], axis=0).astype(bf16)
        contract = (((1,), (1,)), ((), ()))
        found = lax.dot_general(lhs_high, stacked, contract, preferred_element_type=f32)
        found = found + lax.dot_general(lhs_low, stacked, contract, preferred_element_type=f32)
        return lift, found

    def placed(lift, found):
        wide = jnp.concatenate([found, jnp.zeros((64, 112), f32)], axis=1)
        folded = pltpu.roll(wide, lift, 1) + pltpu.roll(wide, (lift + 120) & 127, 1)
        lane = lane_iota(64)
        return jnp.where((lane >= lift) & (lane < lift + 8), folded, 0.0)

    def to_bricks(step, carry):
        blocks = [(BLOCKS - 1) - (step * p2g_batch + u) for u in range(p2g_batch)]
        sums_of = [brick_sums(b) for b in blocks]
        out = [placed(*found) for found in sums_of]
        for b, value in zip(blocks, out):
            chain[b] = value + chain[following(b)]
        return carry

    lax.fori_loop(0, BLOCKS // p2g_batch, to_bricks, 0)

    def spread(p, carry):
        for q in range(9):
            cells = [[first_of((p + 1 - dp) * 10 + (q + 1 - dq)) for dq in range(2)] for dp in range(2)]
            for x in range(2):
                total = None
                for dp in range(2):
                    for dq in range(2):
                        start = 8 * (2 * (x + 2 * dp) + dq)
                        value = chain[cells[dp][dq], start : start + 8, :]
                        total = value if total is None else total + value
                grid[q, 2 * p + x] = total
        return carry

    lax.fori_loop(0, 9, spread, 0)

    halo_copies = []
    faces = {-1: 0, 1: 1}
    for m, (a, b) in enumerate(move_list):
        xs = pl.ds(16, 2) if a == 1 else pl.ds(0, 2)
        y = 8 if b == 1 else 0
        if b == 0:
            source, target = grid.at[:, xs], face_x.at[faces[a]]
        elif a == 0:
            source, target = grid.at[y], face_y.at[faces[b]]
        else:
            source, target = grid.at[y, xs], corner.at[2 * faces[a] + faces[b]]
        halo_copies.append(remote(source, target, halo_send.at[m], halo_recv.at[m], a, b))
    for m in (3, 4, 0, 2, 5, 7, 1, 6):
        halo_copies[m].start()
    for copy in mask_copies:
        copy.start()
    for m in early_order[early_first:]:
        early_copies[m].start()

    def own_mask(x, carry):
        movable[x, 0:16, :] = (1 - mask_ref[pl.ds(pl.multiple_of(x * 16, 16), 16), :]).astype(f32)
        return carry

    lax.fori_loop(0, 16, own_mask, 0)
    row8 = row_iota(8)
    even = (row8 & 1) == 0
    quantity = row8 // 2
    pull = jnp.where(quantity == 1, time_step * gravity[0], 0.0)
    pull = jnp.where(quantity == 2, time_step * gravity[1], pull)
    pull = jnp.where(quantity == 3, time_step * gravity[2], pull)

    def put_velocity(x, yp, tile):
        mass = jnp.where(row8 < 2, tile, 0.0)
        mass = mass + pltpu.roll(mass, 2, 0)
        mass = mass + pltpu.roll(mass, 4, 0)
        free = jnp.where(even, movable[x, pl.ds(2 * yp, 1), :], movable[x, pl.ds(2 * yp + 1, 1), :])
        node_v[x, yp] = free * (tile / jnp.maximum(mass, mass_floor) + pull)

    def interior(x, carry):
        for yp in range(1, 8):
            put_velocity(x, yp, grid[yp, x])
        return carry

    lax.fori_loop(2, 16, interior, 0)
    for copy in mask_copies:
        copy.wait_recv()
    past_x = inside(1, 0).astype(f32)
    past_y = inside(0, 1).astype(f32)
    past_c = inside(1, 1).astype(f32)
    for xx in range(2):
        movable[16 + xx, 0:16, :] = (1 - mask_x_in[pl.ds(16 * xx, 16), :]).astype(f32) * past_x
        for par in range(2):
            movable[16 + xx, 16 + par : 17 + par, :] = (
                1 - mask_c_in[par, xx : xx + 1, :]
            ).astype(f32) * past_c

    def side_mask(x, carry):
        for par in range(2):
            movable[x, 16 + par : 17 + par, :] = (1 - mask_y_in[par, pl.ds(x, 1), :]).astype(f32) * past_y
        return carry

    lax.fori_loop(0, 16, side_mask, 0)
    for copy in halo_copies:
        copy.wait_recv()

    def low_high(yp):
        for a in (-1, 1):
            for xx in range(2):
                x = xx if a == 1 else 16 + xx
                yield a, xx, x, grid[yp, x] + face_x[faces[a], yp, xx]

    def edge_x(yp, carry):
        for _, _, x, tile in low_high(yp):
            put_velocity(x, yp, tile)
        return carry

    lax.fori_loop(1, 8, edge_x, 0)

    def edge_y(x, carry):
        for b in (-1, 1):
            yp = 0 if b == 1 else 8
            put_velocity(x, yp, grid[yp, x] + face_y[faces[b], x])
        return carry

    lax.fori_loop(2, 16, edge_y, 0)
    for b in (-1, 1):
        yp = 0 if b == 1 else 8
        for a, xx, x, tile in low_high(yp):
            tile = tile + face_y[faces[b], x]
            tile = tile + corner[2 * faces[a] + faces[b], xx]
            put_velocity(x, yp, tile)

    lane8 = lane_iota(8)

    def brick_tiles(b):
        column = column_of(b)
        p = column // NBY
        q = lax.rem(column, NBY)
        return [node_v[2 * p + x, q + yp] for x in range(4) for yp in range(2)]

    for move in early_order:
        packed = [jnp.zeros((8, 128), f32)] * 4
        for k in range(8):
            b = source_of(move * 8 + k)
            lift = lift_of(b)
            tiles = brick_tiles(b)
            shift = (8 * k + 128 - lift) & 127
            local = lane8 - 8 * k
            low = (local >= 0) & (local < 8) & (local + lift < GZ)
            local = local - 64
            high = (local >= 0) & (local < 8) & (local + lift < GZ)
            for t in range(4):
                kept = jnp.where(low, pltpu.roll(tiles[t], shift, 1), packed[t])
                packed[t] = jnp.where(high, pltpu.roll(tiles[t + 4], (shift + 64) & 127, 1), kept)
        for t in range(3):
            moved = pltpu.roll(packed[3], (8 - (2 + 2 * t)) & 7, 0)
            late[move, t] = jnp.where(row8 < 2, moved, packed[t])
        late_copies[move].start()

    lane64 = lane_iota(64)

    def windows(stack, shift):
        first = pltpu.roll(stack, shift & 127, 1)
        second = pltpu.roll(stack, (shift + 8) & 127, 1)
        third = pltpu.roll(stack, (shift + 16) & 127, 1)
        return jnp.where(lane64 < 8, first, jnp.where(lane64 < 16, second, third))

    def put_sums(b, total):
        base = pl.multiple_of(b * 32, 32)
        for t in range(4):
            sums[pl.ds(base + 8 * t, 8), :] = total[t]

    def resident(step, carry):
        blocks = [step * g2p_batch + u for u in range(g2p_batch)]
        totals = []
        for b in blocks:
            lift = lift_of(b)
            stack = jnp.concatenate(brick_tiles(b), axis=0)
            totals.append(
                gathered(
                    windows(stack, 128 - lift),
                    pos_ref[0, pl.ds(b, 1), :],
                    pos_ref[1, pl.ds(b, 1), :],
                    pos_ref[2, pl.ds(b, 1), :],
                    GZ - lift,
                )
            )
        for b, total in zip(blocks, totals):
            put_sums(b, total)
        return carry

    lax.fori_loop(0, BLOCKS // g2p_batch, resident, 0)

    def finish(g, carry):
        rows = pl.ds(pl.multiple_of(g * 8, 8), 8)
        position = [pos_ref[c, rows, :] for c in range(3)]
        deform = [def_ref[c, rows, :] for c in range(9)]
        keep = jnp.where(mass_ref[rows, :] > 0.0, stay_ref[rows, :], 0.0)
        for row, value in enumerate(final_rows(sums, g * 256, position, deform)):
            state_ref[row, rows, :] = value * keep
        return carry

    lax.fori_loop(0, 8, finish, 0)
    stores = [pltpu.make_async_copy(state_ref, state_out, out_sem.at[8])]
    stores[0].start()

    for move in arrival_order:
        a, b = move_list[move]
        early_copies[move].wait_recv()
        late_copies[move].wait_recv()
        rows = pl.ds(move * 8, 8)

        @pl.when(jnp.logical_not(inside(-a, -b)))
        def nobody(rows=rows):
            arrive_ref[:, rows, :] = jnp.zeros((25, 8, 128), f32)

        @pl.when(inside(-a, -b))
        def somebody(move=move, rows=rows):
            packed = [late_in[move, t] for t in range(3)]
            last = jnp.zeros((8, 128), f32)
            for t in range(3):
                last = last + pltpu.roll(jnp.where(row8 < 2, packed[t], 0.0), 2 + 2 * t, 0)
            packed.append(last)
            low_stack = jnp.concatenate(packed, axis=0)
            stack = jnp.concatenate([low_stack, pltpu.roll(low_stack, 64, 1)], axis=0)

            def arriving(step, carry, move=move, stack=stack):
                ks = [step * g2p_batch + u for u in range(g2p_batch)]
                totals = [
                    gathered(
                        windows(stack, 128 - 8 * k),
                        early_in[move, 0, pl.ds(k, 1), :],
                        early_in[move, 1, pl.ds(k, 1), :],
                        early_in[move, 2, pl.ds(k, 1), :],
                        None,
                    )
                    for k in ks
                ]
                for k, total in zip(ks, totals):
                    put_sums(k, total)
                return carry

            lax.fori_loop(0, 8 // g2p_batch, arriving, 0)
            position = [early_in[move, c] for c in range(3)]
            deform = [early_in[move, 3 + c] for c in range(9)]
            mass = early_in[move, 12]
            keep = jnp.where(mass > 0.0, 1.0, 0.0)
            for row, value in enumerate(final_rows(sums, 0, position, deform)):
                arrive_ref[row, rows, :] = value * keep
            arrive_ref[24, rows, :] = mass

        store = pltpu.make_async_copy(arrive_ref.at[:, rows], arrive_out.at[:, rows], out_sem.at[move])
        store.start()
        stores.append(store)
    for copy in early_copies + late_copies + halo_copies + mask_copies:
        copy.wait_send()
    for store in stores:
        store.wait()


def pass_on(state, arrivals, state_out, arrive_out, held, held_too, in_sem, out_sem):
    chunks = [(state, held, state_out, pl.ds(6 * n, 6)) for n in range(4)]
    chunks += [(arrivals, held_too, arrive_out, pl.ds(5 * n, 5)) for n in range(5)]
    taken = [pltpu.make_async_copy(a.at[d], v.at[d], in_sem.at[n]) for n, (a, v, _, d) in enumerate(chunks)]
    given = [pltpu.make_async_copy(v.at[d], o.at[d], out_sem.at[n]) for n, (_, v, o, d) in enumerate(chunks)]
    for copy in taken:
        copy.start()
    for copy, onward in zip(taken, given):
        copy.wait()
        onward.start()
    for onward in given:
        onward.wait()


def body(
    n_down,
    n_cross,
    position,
    velocity,
    affine,
    deform,
    particle_mass,
    block_count,
    block_brick,
    boundary_mask,
    leaving_block,
    leaving_dest,
):
    vmem = pl.BlockSpec(memory_space=pltpu.VMEM)
    dma = pltpu.SemaphoreType.DMA
    hbm = pl.BlockSpec(memory_space=pltpu.HBM)
    results = pl.pallas_call(
        functools.partial(kernel, n_down, n_cross),
        out_shape=(
            jax.ShapeDtypeStruct((24, BLOCKS, SLOTS), f32),
            jax.ShapeDtypeStruct((25, BLOCKS, SLOTS), f32),
        ),
        in_specs=[vmem] * 4 + [pl.BlockSpec(memory_space=pltpu.HBM)] * 6,
        out_specs=(hbm, hbm),
        scratch_shapes=[
            pltpu.VMEM((3, BLOCKS, SLOTS), f32),
            pltpu.VMEM((3, BLOCKS, SLOTS), f32),
            pltpu.VMEM((9, BLOCKS, SLOTS), f32),
            pltpu.VMEM((9, BLOCKS, SLOTS), f32),
            pltpu.VMEM((BLOCKS, SLOTS), f32),
            pltpu.VMEM((GX * GY, GZ), jnp.int32),
            dma((6,)),
            pltpu.VMEM((24, BLOCKS, SLOTS), f32),
            pltpu.VMEM((25, BLOCKS, SLOTS), f32),
            dma((9,)),
            pltpu.VMEM((8, 13, 8, 128), f32),
            pltpu.VMEM((8, 13, 8, 128), f32),
            pltpu.VMEM((8, 3, 8, 128), f32),
            pltpu.VMEM((8, 3, 8, 128), f32),
            pltpu.VMEM((BLOCKS * 32, 128), f32),
            pltpu.VMEM((BLOCKS + 1, 64, 128), f32),
            pltpu.VMEM((9, 18, 8, 128), f32),
            pltpu.VMEM((18, 9, 8, 128), f32),
            pltpu.VMEM((18, 24, 128), f32),
            pltpu.VMEM((2, 16, 128), jnp.int32),
            pltpu.VMEM((32, 128), jnp.int32),
            pltpu.VMEM((2, 16, 128), jnp.int32),
            pltpu.VMEM((2, 8, 128), jnp.int32),
            pltpu.VMEM((2, 9, 2, 8, 128), f32),
            pltpu.VMEM((2, 18, 8, 128), f32),
            pltpu.VMEM((4, 2, 8, 128), f32),
            pltpu.VMEM((BLOCKS * 32, 128), f32),
            pltpu.VMEM((BLOCKS, SLOTS), f32),
            pltpu.VMEM((BLOCKS, SLOTS), f32),
            pltpu.VMEM((8, 128), jnp.int32),
            pltpu.SMEM((8, 128), jnp.int32),
            dma,
            dma((8,)),
            dma((8,)),
            dma((8,)),
            dma((8,)),
            dma((8,)),
            dma((8,)),
            dma((3,)),
            dma((3,)),
        ],
        compiler_params=pltpu.CompilerParams(collective_id=0, has_side_effects=True),
    )(
        block_count.reshape(1, BLOCKS),
        block_brick.reshape(1, BLOCKS),
        leaving_block.reshape(1, BLOCKS),
        leaving_dest.reshape(1, BLOCKS),
        position,
        velocity,
        affine,
        deform,
        particle_mass,
        boundary_mask.reshape(GX * GY, GZ),
    )
    return pl.pallas_call(
        pass_on,
        out_shape=(
            jax.ShapeDtypeStruct((24, BLOCKS, SLOTS), f32),
            jax.ShapeDtypeStruct((25, BLOCKS, SLOTS), f32),
        ),
        in_specs=[hbm, hbm],
        out_specs=(hbm, hbm),
        scratch_shapes=[
            pltpu.VMEM((24, BLOCKS, SLOTS), f32),
            pltpu.VMEM((25, BLOCKS, SLOTS), f32),
            dma((9,)),
            dma((9,)),
        ],
    )(*results)


def solution(mesh):
    blocks = P(None, ("down", "cross"), None)
    flat = P(("down", "cross"))
    in_specs = (
        blocks,
        blocks,
        blocks,
        blocks,
        P(("down", "cross"), None),
        flat,
        flat,
        P("down", "cross", None),
        flat,
        flat,
    )
    step = functools.partial(body, mesh.shape["down"], mesh.shape["cross"])
    return jax.shard_map(step, mesh=mesh, in_specs=in_specs, out_specs=(blocks, blocks), check_vma=False)
```

```python
import functools

import jax
import jax.numpy as jnp
from jax import lax
from jax.experimental import pallas as pl
from jax.experimental.pallas import tpu as pltpu
from jax.sharding import PartitionSpec as P

GX = 16
GY = 16
GZ = 128
SLOTS = 128
BLOCKS = 64
MIG = 8
NBX = 8
NBY = 8

time_step = 0.05
shear_modulus = 8.0
lame_first = 12.0
stress_factor = 0.2
gravity = (2.0, 0.0, -9.0)
mass_floor = 1.0
move_list = ((-1, -1), (-1, 0), (-1, 1), (0, -1), (0, 1), (1, -1), (1, 0), (1, 1))
early_order = (0, 2, 1, 6, 5, 7, 3, 4)
arrival_order = (1, 6, 0, 2, 5, 7, 3, 4)
early_first = 6
late_order = (0, 2, 5, 7, 3, 4, 1, 6)
p2g_batch = 8
g2p_batch = 8

MESH = pl.DeviceIdType.MESH
f32 = jnp.float32
bf16 = jnp.bfloat16


def spline(distance):
    magnitude = jnp.abs(distance)
    outer_part = jnp.maximum(1.5 - magnitude, 0.0)
    return jnp.where(magnitude < 0.5, 0.75 - magnitude * magnitude, 0.5 * outer_part * outer_part)


def row_iota(rows):
    return lax.broadcasted_iota(jnp.int32, (rows, 128), 0)


def lane_iota(rows):
    return lax.broadcasted_iota(jnp.int32, (rows, 128), 1)


def plane_weights(x0, x1):
    parity = (row_iota(8) & 1).astype(f32)
    dx = [float(x) - x0 for x in range(4)]
    wx = [spline(d) for d in dx]
    dy = [(parity + 2.0 * yp) - x1 for yp in range(2)]
    wy = [spline(d) for d in dy]
    return dx, wx, dy, wy


def split(value):
    high = value.astype(bf16)
    low = (value - high.astype(f32)).astype(bf16)
    return high, low


def particle_rows(deform, affine, velocity, mass):
    d = deform
    determinant = (
        d[0] * (d[4] * d[8] - d[5] * d[7])
        - d[1] * (d[3] * d[8] - d[5] * d[6])
        + d[2] * (d[3] * d[7] - d[4] * d[6])
    )
    pressure = lame_first * jnp.log(determinant)
    columns = [[None] * 3 for _ in range(3)]
    for a in range(3):
        for c in range(a, 3):
            product = d[3 * a] * d[3 * c] + d[3 * a + 1] * d[3 * c + 1] + d[3 * a + 2] * d[3 * c + 2]
            if a == c:
                tau = shear_modulus * (product - 1.0) + pressure
            else:
                tau = shear_modulus * product
            columns[c][a] = mass * (affine[3 * a + c] - stress_factor * tau)
            if a != c:
                columns[a][c] = mass * (affine[3 * c + a] - stress_factor * tau)
    return [mass] + [mass * v for v in velocity], columns


def gathered(lhs_f32, x0, x1, x2, limit):
    lane = lane_iota(64)
    high = lhs_f32.astype(bf16).astype(f32)
    low = lhs_f32 - high
    lhs = jnp.where((lane >= 8) & (lane < 16), low, high)
    lhs = jnp.where(lane < 24, lhs, 0.0).astype(bf16)
    height = row_iota(8)
    dz = height.astype(f32) - x2
    wz = spline(dz)
    if limit is not None:
        wz = jnp.where(height < limit, wz, 0.0)
    rhs = jnp.concatenate([wz, wz * dz], axis=1)
    rhs_high = rhs.astype(bf16).astype(f32)
    rhs_low = rhs - rhs_high
    stacked = jnp.concatenate([rhs_high, rhs_high, rhs_low, jnp.zeros_like(rhs)], axis=0).astype(bf16)
    u = jnp.dot(lhs[:, :32], stacked, preferred_element_type=f32)
    dx, wx, dy, wy = plane_weights(x0, x1)
    wyd = [w * d for w, d in zip(wy, dy)]
    total = None
    for x in range(4):
        a = b = c = None
        for yp in range(2):
            start = 8 * (2 * x + yp)
            u0 = u[start : start + 8, :128]
            u1 = u[start : start + 8, 128:]
            terms = (wy[yp] * u0, wyd[yp] * u0, wy[yp] * u1)
            a, b, c = terms if a is None else (a + terms[0], b + terms[1], c + terms[2])
        parts = (wx[x] * a, (wx[x] * dx[x]) * a, wx[x] * b, wx[x] * c)
        total = parts if total is None else tuple(t + p for t, p in zip(total, parts))
    return total


def final_rows(sums_ref, base, position, deform):
    def both(row):
        return sums_ref[pl.ds(base + row, 8, stride=32), :] + sums_ref[pl.ds(base + row + 1, 8, stride=32), :]

    v = [both(2 + 2 * a) for a in range(3)]
    c = [4.0 * both(8 * (1 + col) + 2 + 2 * a) for a in range(3) for col in range(3)]
    x = [position[a] + time_step * v[a] for a in range(3)]
    f = []
    for a in range(3):
        for col in range(3):
            grown = c[3 * a] * deform[col] + c[3 * a + 1] * deform[3 + col] + c[3 * a + 2] * deform[6 + col]
            f.append(deform[3 * a + col] + time_step * grown)
    return x + v + c + f


def build_tables(count_ref, brick_ref, leave_ref, dest_ref, weight_ref, mass_ref, stay_ref, staged):
    shape = (128, 128)
    down = lax.broadcasted_iota(jnp.int32, shape, 0)
    across = lax.broadcasted_iota(jnp.int32, shape, 1)

    def padded(row, filler):
        return jnp.concatenate([row, jnp.full((1, 128 - BLOCKS), filler, jnp.int32)], axis=1)

    def upright(row):
        return jnp.transpose(jnp.broadcast_to(row, shape))

    def least(value):
        return jnp.min(value, axis=0, keepdims=True)

    count = upright(padded(count_ref[...], 0))[:BLOCKS]
    lane = across[:BLOCKS]
    mass_ref[...] = jnp.where(lane < count, weight_ref[...], 0.0)
    brick = padded(brick_ref[...], 0)
    column = brick >> 5
    sides = upright(column)[:BLOCKS]
    ids = down[:BLOCKS]
    staged[0:1, :] = least(jnp.where((sides == column) & (ids > lane), ids, BLOCKS))
    cell = ((sides >> 3) + 1) * 10 + (sides & 7) + 1
    staged[1:2, :] = least(jnp.where(cell == lane, ids, BLOCKS))
    staged[2:3, :] = column
    staged[3:4, :] = (brick & 31) * 4
    leave = padded(leave_ref[...], 0)
    dest = padded(dest_ref[...], 4)
    dest_up = upright(dest)[:BLOCKS]
    leave_up = upright(leave)[:BLOCKS]
    rank = jnp.sum(jnp.where((dest_up == dest) & (ids < lane), 1, 0), axis=0, keepdims=True)
    move = jnp.where(dest > 4, dest - 1, dest)
    slot = jnp.where(dest == 4, -1, move * 8 + rank)
    slot_up = upright(slot)[:BLOCKS]
    match = slot_up == lane
    staged[4:5, :] = jnp.sum(jnp.where(match, leave_up, 0), axis=0, keepdims=True)
    staged[5:6, :] = jnp.sum(jnp.where(match, 1, 0), axis=0, keepdims=True)
    staged[6:8, :] = jnp.zeros((2, 128), jnp.int32)
    gone = jnp.where((leave == ids) & (dest != 4), 1.0, 0.0)
    stay_ref[...] = jnp.broadcast_to(1.0 - jnp.max(gone, axis=1, keepdims=True), (BLOCKS, SLOTS))


def kernel(
    n_down,
    n_cross,
    count_ref,
    brick_ref,
    leave_ref,
    dest_ref,
    pos_hbm,
    vel_hbm,
    aff_hbm,
    def_hbm,
    weight_hbm,
    mask_hbm,
    state_out,
    arrive_out,
    pos_ref,
    vel_ref,
    aff_ref,
    def_ref,
    weight_ref,
    mask_ref,
    load_sem,
    state_ref,
    arrive_ref,
    out_sem,
    early,
    early_in,
    late,
    late_in,
    table,
    chain,
    grid,
    node_v,
    movable,
    mask_y,
    mask_x_in,
    mask_y_in,
    mask_c_in,
    face_x,
    face_y,
    corner,
    sums,
    mass_ref,
    stay_ref,
    staged,
    scalars,
    scalar_sem,
    early_send,
    early_recv,
    late_send,
    late_recv,
    halo_send,
    halo_recv,
    mask_send,
    mask_recv,
):
    loads = [
        pltpu.make_async_copy(source, target, load_sem.at[n])
        for n, (source, target) in enumerate(
            (
                (weight_hbm, weight_ref),
                (mask_hbm, mask_ref),
                (pos_hbm, pos_ref),
                (def_hbm, def_ref),
                (vel_hbm, vel_ref),
                (aff_hbm, aff_ref),
            )
        )
    ]
    for load in loads:
        load.start()
    i = lax.axis_index("down")
    j = lax.axis_index("cross")

    def device(a, b):
        return (lax.rem(i + (a + n_down), n_down), lax.rem(j + (b + n_cross), n_cross))

    def inside(a, b):
        valid = None
        if a:
            valid = (i + a >= 0) & (i + a < n_down)
        if b:
            other = (j + b >= 0) & (j + b < n_cross)
            valid = other if valid is None else valid & other
        return valid

    class Edge:
        def __init__(self, copy, a, b):
            self.copy, self.a, self.b = copy, a, b

        def start(self):
            pl.when(inside(self.a, self.b))(self.copy.start)

        def wait_send(self):
            pl.when(inside(self.a, self.b))(self.copy.wait_send)

        def wait_recv(self):
            pl.when(inside(-self.a, -self.b))(self.copy.wait_recv)

    barrier = pltpu.get_barrier_semaphore()
    neighbours = 0
    for a, b in move_list:

        @pl.when(inside(a, b))
        def greet(a=a, b=b):
            pl.semaphore_signal(barrier, inc=1, device_id=device(a, b), device_id_type=MESH)

        neighbours = neighbours + inside(a, b).astype(jnp.int32)

    def fill(target, a, b):
        @pl.when(jnp.logical_not(inside(a, b)))
        def zeros():
            target[...] = jnp.zeros(target.shape, target.dtype)

    for sign in (-1, 1):
        fill(face_x.at[(sign + 1) // 2], -sign, 0)
        fill(face_y.at[(sign + 1) // 2], 0, -sign)
        for other in (-1, 1):
            fill(corner.at[sign + 1 + (other + 1) // 2], -sign, -other)
    fill(mask_x_in, 1, 0)
    fill(mask_y_in, 0, 1)
    fill(mask_c_in, 1, 1)

    loads[0].wait()
    build_tables(count_ref, brick_ref, leave_ref, dest_ref, weight_ref, mass_ref, stay_ref, staged)
    to_scalars = pltpu.make_async_copy(staged, scalars, scalar_sem)
    to_scalars.start()
    loads[1].wait()
    for par in range(2):
        mask_y[par] = mask_ref[pl.ds(par, 16, stride=16), :]
    to_scalars.wait()
    loads[2].wait()
    loads[3].wait()
    following = lambda b: scalars[0, b]
    first_of = lambda cell: scalars[1, cell]
    column_of = lambda b: scalars[2, b]
    lift_of = lambda b: scalars[3, b]
    source_of = lambda slot: scalars[4, slot]
    present_of = lambda slot: scalars[5, slot]

    def pick(move, carry):
        for k in range(8):
            source = source_of(move * 8 + k)
            early[move, 0:3, k : k + 1, :] = pos_ref[:, pl.ds(source, 1), :]
            early[move, 3:12, k : k + 1, :] = def_ref[:, pl.ds(source, 1), :]
            here = present_of(move * 8 + k).astype(f32)
            early[move, 12, k : k + 1, :] = mass_ref[pl.ds(source, 1), :] * here
        return carry

    lax.fori_loop(0, 8, pick, 0)

    def remote(source, target, send, recv, a, b):
        copy = pltpu.make_async_remote_copy(
            src_ref=source,
            dst_ref=target,
            send_sem=send,
            recv_sem=recv,
            device_id=device(a, b),
            device_id_type=MESH,
        )
        return Edge(copy, a, b)

    early_copies = [
        remote(early.at[m], early_in.at[m], early_send.at[m], early_recv.at[m], a, b)
        for m, (a, b) in enumerate(move_list)
    ]
    late_copies = [
        remote(late.at[m], late_in.at[m], late_send.at[m], late_recv.at[m], a, b)
        for m, (a, b) in enumerate(move_list)
    ]
    mask_copies = [
        remote(mask_y, mask_y_in, mask_send.at[0], mask_recv.at[0], 0, -1),
        remote(mask_ref.at[pl.ds(0, 32)], mask_x_in, mask_send.at[1], mask_recv.at[1], -1, 0),
        remote(mask_y.at[:, pl.ds(0, 8)], mask_c_in, mask_send.at[2], mask_recv.at[2], -1, -1),
    ]

    pl.semaphore_wait(barrier, neighbours)
    for m in early_order[:early_first]:
        early_copies[m].start()

    def terms(g, carry):
        rows = pl.ds(pl.multiple_of(g * 8, 8), 8)
        deform = [def_ref[c, rows, :] for c in range(9)]
        affine = [aff_ref[c, rows, :] for c in range(9)]
        velocity = [vel_ref[c, rows, :] for c in range(3)]
        moved, columns = particle_rows(deform, affine, velocity, mass_ref[rows, :])
        zero = jnp.zeros((8, 128), f32)
        lists = [moved] + [[zero] + columns[c] for c in range(3)]
        for group, values in enumerate(lists):
            for quantity, value in enumerate(values):
                for par in range(2):
                    row = g * 256 + (8 * group + 2 * quantity + par)
                    table[pl.ds(row, 8, stride=32), :] = value
        return carry

    loads[4].wait()
    loads[5].wait()
    lax.fori_loop(0, 8, terms, 0)

    chain[BLOCKS] = jnp.zeros((64, 128), f32)

    def brick_sums(b):
        lift = lift_of(b)
        x0 = pos_ref[0, pl.ds(b, 1), :]
        x1 = pos_ref[1, pl.ds(b, 1), :]
        x2 = pos_ref[2, pl.ds(b, 1), :]
        base = pl.multiple_of(b * 32, 32)
        moved = table[pl.ds(base, 8), :]
        col0 = table[pl.ds(base + 8, 8), :]
        col1 = table[pl.ds(base + 16, 8), :]
        col2 = table[pl.ds(base + 24, 8), :]
        dx, wx, dy, wy = plane_weights(x0, x1)
        plain, raised = [], []
        for x in range(4):
            at_x = moved + col0 * dx[x]
            for yp in range(2):
                weight = wx[x] * wy[yp]
                plain.append((at_x + col1 * dy[yp]) * weight)
                raised.append(col2 * weight)
        lhs = jnp.concatenate([jnp.concatenate(plain, axis=0), jnp.concatenate(raised, axis=0)], axis=1)
        lhs_high, lhs_low = split(lhs)
        height = row_iota(8)
        dz = height.astype(f32) - x2
        wz = jnp.where(height + lift < GZ, spline(dz), 0.0)
        rhs = jnp.concatenate([wz, wz * dz], axis=1)
        rhs_high = rhs.astype(bf16).astype(f32)
        stacked = jnp.concatenate([rhs_high, rhs - rhs_high], axis=0).astype(bf16)
        contract = (((1,), (1,)), ((), ()))
        found = lax.dot_general(lhs_high, stacked, contract, preferred_element_type=f32)
        found = found + lax.dot_general(lhs_low, stacked, contract, preferred_element_type=f32)
        return lift, found

    def placed(lift, found):
        wide = jnp.concatenate([found, jnp.zeros((64, 112), f32)], axis=1)
        folded = pltpu.roll(wide, lift, 1) + pltpu.roll(wide, (lift + 120) & 127, 1)
        lane = lane_iota(64)
        return jnp.where((lane >= lift) & (lane < lift + 8), folded, 0.0)

    def to_bricks(step, carry):
        blocks = [(BLOCKS - 1) - (step * p2g_batch + u) for u in range(p2g_batch)]
        sums_of = [brick_sums(b) for b in blocks]
        out = [placed(*found) for found in sums_of]
        for b, value in zip(blocks, out):
            chain[b] = value + chain[following(b)]
        return carry

    lax.fori_loop(0, BLOCKS // p2g_batch, to_bricks, 0)

    def spread(p, carry):
        for q in range(9):
            cells = [[first_of((p + 1 - dp) * 10 + (q + 1 - dq)) for dq in range(2)] for dp in range(2)]
            for x in range(2):
                total = None
                for dp in range(2):
                    for dq in range(2):
                        start = 8 * (2 * (x + 2 * dp) + dq)
                        value = chain[cells[dp][dq], start : start + 8, :]
                        total = value if total is None else total + value
                grid[q, 2 * p + x] = total
        return carry

    lax.fori_loop(0, 9, spread, 0)

    halo_copies = []
    faces = {-1: 0, 1: 1}
    for m, (a, b) in enumerate(move_list):
        xs = pl.ds(16, 2) if a == 1 else pl.ds(0, 2)
        y = 8 if b == 1 else 0
        if b == 0:
            source, target = grid.at[:, xs], face_x.at[faces[a]]
        elif a == 0:
            source, target = grid.at[y], face_y.at[faces[b]]
        else:
            source, target = grid.at[y, xs], corner.at[2 * faces[a] + faces[b]]
        halo_copies.append(remote(source, target, halo_send.at[m], halo_recv.at[m], a, b))
    for m in (3, 4, 0, 2, 5, 7, 1, 6):
        halo_copies[m].start()
    for copy in mask_copies:
        copy.start()
    for m in early_order[early_first:]:
        early_copies[m].start()

    def own_mask(x, carry):
        movable[x, 0:16, :] = (1 - mask_ref[pl.ds(pl.multiple_of(x * 16, 16), 16), :]).astype(f32)
        return carry

    lax.fori_loop(0, 16, own_mask, 0)
    row8 = row_iota(8)
    even = (row8 & 1) == 0
    quantity = row8 // 2
    pull = jnp.where(quantity == 1, time_step * gravity[0], 0.0)
    pull = jnp.where(quantity == 2, time_step * gravity[1], pull)
    pull = jnp.where(quantity == 3, time_step * gravity[2], pull)

    def put_velocity(x, yp, tile):
        mass = jnp.where(row8 < 2, tile, 0.0)
        mass = mass + pltpu.roll(mass, 2, 0)
        mass = mass + pltpu.roll(mass, 4, 0)
        free = jnp.where(even, movable[x, pl.ds(2 * yp, 1), :], movable[x, pl.ds(2 * yp + 1, 1), :])
        node_v[x, yp] = free * (tile / jnp.maximum(mass, mass_floor) + pull)

    def interior(x, carry):
        for yp in range(1, 8):
            put_velocity(x, yp, grid[yp, x])
        return carry

    lax.fori_loop(2, 16, interior, 0)
    for copy in mask_copies:
        copy.wait_recv()
    past_x = inside(1, 0).astype(f32)
    past_y = inside(0, 1).astype(f32)
    past_c = inside(1, 1).astype(f32)
    for xx in range(2):
        movable[16 + xx, 0:16, :] = (1 - mask_x_in[pl.ds(16 * xx, 16), :]).astype(f32) * past_x
        for par in range(2):
            movable[16 + xx, 16 + par : 17 + par, :] = (
                1 - mask_c_in[par, xx : xx + 1, :]
            ).astype(f32) * past_c

    def side_mask(x, carry):
        for par in range(2):
            movable[x, 16 + par : 17 + par, :] = (1 - mask_y_in[par, pl.ds(x, 1), :]).astype(f32) * past_y
        return carry

    lax.fori_loop(0, 16, side_mask, 0)
    for copy in halo_copies:
        copy.wait_recv()

    def low_high(yp):
        for a in (-1, 1):
            for xx in range(2):
                x = xx if a == 1 else 16 + xx
                yield a, xx, x, grid[yp, x] + face_x[faces[a], yp, xx]

    def edge_x(yp, carry):
        for _, _, x, tile in low_high(yp):
            put_velocity(x, yp, tile)
        return carry

    lax.fori_loop(1, 8, edge_x, 0)

    def edge_y(x, carry):
        for b in (-1, 1):
            yp = 0 if b == 1 else 8
            put_velocity(x, yp, grid[yp, x] + face_y[faces[b], x])
        return carry

    lax.fori_loop(2, 16, edge_y, 0)
    for b in (-1, 1):
        yp = 0 if b == 1 else 8
        for a, xx, x, tile in low_high(yp):
            tile = tile + face_y[faces[b], x]
            tile = tile + corner[2 * faces[a] + faces[b], xx]
            put_velocity(x, yp, tile)

    lane8 = lane_iota(8)

    def brick_tiles(b):
        column = column_of(b)
        p = column // NBY
        q = lax.rem(column, NBY)
        return [node_v[2 * p + x, q + yp] for x in range(4) for yp in range(2)]

    for move in late_order:
        packed = [jnp.zeros((8, 128), f32)] * 4
        for k in range(8):
            b = source_of(move * 8 + k)
            lift = lift_of(b)
            tiles = brick_tiles(b)
            shift = (8 * k + 128 - lift) & 127
            local = lane8 - 8 * k
            low = (local >= 0) & (local < 8) & (local + lift < GZ)
            local = local - 64
            high = (local >= 0) & (local < 8) & (local + lift < GZ)
            for t in range(4):
                kept = jnp.where(low, pltpu.roll(tiles[t], shift, 1), packed[t])
                packed[t] = jnp.where(high, pltpu.roll(tiles[t + 4], (shift + 64) & 127, 1), kept)
        for t in range(3):
            moved = pltpu.roll(packed[3], (8 - (2 + 2 * t)) & 7, 0)
            late[move, t] = jnp.where(row8 < 2, moved, packed[t])
        late_copies[move].start()

    lane64 = lane_iota(64)

    def windows(stack, shift):
        first = pltpu.roll(stack, shift & 127, 1)
        second = pltpu.roll(stack, (shift + 8) & 127, 1)
        third = pltpu.roll(stack, (shift + 16) & 127, 1)
        return jnp.where(lane64 < 8, first, jnp.where(lane64 < 16, second, third))

    def put_sums(b, total):
        base = pl.multiple_of(b * 32, 32)
        for t in range(4):
            sums[pl.ds(base + 8 * t, 8), :] = total[t]

    def resident(step, carry):
        blocks = [step * g2p_batch + u for u in range(g2p_batch)]
        totals = []
        for b in blocks:
            lift = lift_of(b)
            stack = jnp.concatenate(brick_tiles(b), axis=0)
            totals.append(
                gathered(
                    windows(stack, 128 - lift),
                    pos_ref[0, pl.ds(b, 1), :],
                    pos_ref[1, pl.ds(b, 1), :],
                    pos_ref[2, pl.ds(b, 1), :],
                    GZ - lift,
                )
            )
        for b, total in zip(blocks, totals):
            put_sums(b, total)
        return carry

    lax.fori_loop(0, BLOCKS // g2p_batch, resident, 0)

    def finish(g, carry):
        rows = pl.ds(pl.multiple_of(g * 8, 8), 8)
        position = [pos_ref[c, rows, :] for c in range(3)]
        deform = [def_ref[c, rows, :] for c in range(9)]
        keep = jnp.where(mass_ref[rows, :] > 0.0, stay_ref[rows, :], 0.0)
        for row, value in enumerate(final_rows(sums, g * 256, position, deform)):
            state_ref[row, rows, :] = value * keep
        return carry

    lax.fori_loop(0, 8, finish, 0)
    stores = [pltpu.make_async_copy(state_ref, state_out, out_sem.at[8])]
    stores[0].start()

    for move in arrival_order:
        a, b = move_list[move]
        early_copies[move].wait_recv()
        late_copies[move].wait_recv()
        rows = pl.ds(move * 8, 8)

        @pl.when(jnp.logical_not(inside(-a, -b)))
        def nobody(rows=rows):
            arrive_ref[:, rows, :] = jnp.zeros((25, 8, 128), f32)

        @pl.when(inside(-a, -b))
        def somebody(move=move, rows=rows):
            packed = [late_in[move, t] for t in range(3)]
            last = jnp.zeros((8, 128), f32)
            for t in range(3):
                last = last + pltpu.roll(jnp.where(row8 < 2, packed[t], 0.0), 2 + 2 * t, 0)
            packed.append(last)
            low_stack = jnp.concatenate(packed, axis=0)
            stack = jnp.concatenate([low_stack, pltpu.roll(low_stack, 64, 1)], axis=0)

            def arriving(step, carry, move=move, stack=stack):
                ks = [step * g2p_batch + u for u in range(g2p_batch)]
                totals = [
                    gathered(
                        windows(stack, 128 - 8 * k),
                        early_in[move, 0, pl.ds(k, 1), :],
                        early_in[move, 1, pl.ds(k, 1), :],
                        early_in[move, 2, pl.ds(k, 1), :],
                        None,
                    )
                    for k in ks
                ]
                for k, total in zip(ks, totals):
                    put_sums(k, total)
                return carry

            lax.fori_loop(0, 8 // g2p_batch, arriving, 0)
            position = [early_in[move, c] for c in range(3)]
            deform = [early_in[move, 3 + c] for c in range(9)]
            mass = early_in[move, 12]
            keep = jnp.where(mass > 0.0, 1.0, 0.0)
            for row, value in enumerate(final_rows(sums, 0, position, deform)):
                arrive_ref[row, rows, :] = value * keep
            arrive_ref[24, rows, :] = mass

        store = pltpu.make_async_copy(arrive_ref.at[:, rows], arrive_out.at[:, rows], out_sem.at[move])
        store.start()
        stores.append(store)
    for copy in early_copies + late_copies + halo_copies + mask_copies:
        copy.wait_send()
    for store in stores:
        store.wait()


def pass_on(state, arrivals, state_out, arrive_out, held, held_too, in_sem, out_sem):
    chunks = [(state, held, state_out, pl.ds(12 * n, 12)) for n in range(2)]
    chunks += [(arrivals, held_too, arrive_out, pl.ds(5 * n, 5)) for n in range(5)]
    taken = [pltpu.make_async_copy(a.at[d], v.at[d], in_sem.at[n]) for n, (a, v, _, d) in enumerate(chunks)]
    given = [pltpu.make_async_copy(v.at[d], o.at[d], out_sem.at[n]) for n, (_, v, o, d) in enumerate(chunks)]
    for copy in taken:
        copy.start()
    for copy, onward in zip(taken, given):
        copy.wait()
        onward.start()
    for onward in given:
        onward.wait()


def body(
    n_down,
    n_cross,
    position,
    velocity,
    affine,
    deform,
    particle_mass,
    block_count,
    block_brick,
    boundary_mask,
    leaving_block,
    leaving_dest,
):
    vmem = pl.BlockSpec(memory_space=pltpu.VMEM)
    dma = pltpu.SemaphoreType.DMA
    hbm = pl.BlockSpec(memory_space=pltpu.HBM)
    results = pl.pallas_call(
        functools.partial(kernel, n_down, n_cross),
        out_shape=(
            jax.ShapeDtypeStruct((24, BLOCKS, SLOTS), f32),
            jax.ShapeDtypeStruct((25, BLOCKS, SLOTS), f32),
        ),
        in_specs=[vmem] * 4 + [pl.BlockSpec(memory_space=pltpu.HBM)] * 6,
        out_specs=(hbm, hbm),
        scratch_shapes=[
            pltpu.VMEM((3, BLOCKS, SLOTS), f32),
            pltpu.VMEM((3, BLOCKS, SLOTS), f32),
            pltpu.VMEM((9, BLOCKS, SLOTS), f32),
            pltpu.VMEM((9, BLOCKS, SLOTS), f32),
            pltpu.VMEM((BLOCKS, SLOTS), f32),
            pltpu.VMEM((GX * GY, GZ), jnp.int32),
            dma((6,)),
            pltpu.VMEM((24, BLOCKS, SLOTS), f32),
            pltpu.VMEM((25, BLOCKS, SLOTS), f32),
            dma((9,)),
            pltpu.VMEM((8, 13, 8, 128), f32),
            pltpu.VMEM((8, 13, 8, 128), f32),
            pltpu.VMEM((8, 3, 8, 128), f32),
            pltpu.VMEM((8, 3, 8, 128), f32),
            pltpu.VMEM((BLOCKS * 32, 128), f32),
            pltpu.VMEM((BLOCKS + 1, 64, 128), f32),
            pltpu.VMEM((9, 18, 8, 128), f32),
            pltpu.VMEM((18, 9, 8, 128), f32),
            pltpu.VMEM((18, 24, 128), f32),
            pltpu.VMEM((2, 16, 128), jnp.int32),
            pltpu.VMEM((32, 128), jnp.int32),
            pltpu.VMEM((2, 16, 128), jnp.int32),
            pltpu.VMEM((2, 8, 128), jnp.int32),
            pltpu.VMEM((2, 9, 2, 8, 128), f32),
            pltpu.VMEM((2, 18, 8, 128), f32),
            pltpu.VMEM((4, 2, 8, 128), f32),
            pltpu.VMEM((BLOCKS * 32, 128), f32),
            pltpu.VMEM((BLOCKS, SLOTS), f32),
            pltpu.VMEM((BLOCKS, SLOTS), f32),
            pltpu.VMEM((8, 128), jnp.int32),
            pltpu.SMEM((8, 128), jnp.int32),
            dma,
            dma((8,)),
            dma((8,)),
            dma((8,)),
            dma((8,)),
            dma((8,)),
            dma((8,)),
            dma((3,)),
            dma((3,)),
        ],
        compiler_params=pltpu.CompilerParams(collective_id=0, has_side_effects=True),
    )(
        block_count.reshape(1, BLOCKS),
        block_brick.reshape(1, BLOCKS),
        leaving_block.reshape(1, BLOCKS),
        leaving_dest.reshape(1, BLOCKS),
        position,
        velocity,
        affine,
        deform,
        particle_mass,
        boundary_mask.reshape(GX * GY, GZ),
    )
    return pl.pallas_call(
        pass_on,
        out_shape=(
            jax.ShapeDtypeStruct((24, BLOCKS, SLOTS), f32),
            jax.ShapeDtypeStruct((25, BLOCKS, SLOTS), f32),
        ),
        in_specs=[hbm, hbm],
        out_specs=(hbm, hbm),
        scratch_shapes=[
            pltpu.VMEM((24, BLOCKS, SLOTS), f32),
            pltpu.VMEM((25, BLOCKS, SLOTS), f32),
            dma((7,)),
            dma((7,)),
        ],
    )(*results)


def solution(mesh):
    blocks = P(None, ("down", "cross"), None)
    flat = P(("down", "cross"))
    in_specs = (
        blocks,
        blocks,
        blocks,
        blocks,
        P(("down", "cross"), None),
        flat,
        flat,
        P("down", "cross", None),
        flat,
        flat,
    )
    step = functools.partial(body, mesh.shape["down"], mesh.shape["cross"])
    return jax.shard_map(step, mesh=mesh, in_specs=in_specs, out_specs=(blocks, blocks), check_vma=False)
```
